8 devices in a mesh: batch: 1 (over z), dap: 8 (over y, x, core).
Axes of the slice: x: 2, y: 2, z: 1, core: 2. Of those that a mesh axis runs over, the one named last changes fastest.
Arguments:
- pair_act: bfloat16 [384, 384, 128], P(('batch', 'dap'))
- pair_mask: int32 [384, 384], P(('batch', 'dap'))
- ln_in_scale: bfloat16 [2, 128], replicated
- ln_in_bias: bfloat16 [2, 128], replicated
- w_in: bfloat16 [2, 128, 512], replicated
- b_in: bfloat16 [2, 512], replicated
- w_gate: bfloat16 [2, 128, 128], replicated
- b_gate: bfloat16 [2, 128], replicated
- ln_out_scale: bfloat16 [2, 128], replicated
- ln_out_bias: bfloat16 [2, 128], replicated
- w_out: bfloat16 [2, 128, 128], replicated
- b_out: bfloat16 [2, 128], replicated
Outputs:
- output: bfloat16 [384, 384, 128], P(('batch', 'dap'))
All inputs are finite; a program needn't handle non-finite values.
Results may differ from the reference program's by a relative error of at most 0.00746334.
Values are sent between devices in bfloat16 or wider.
A program may use at most 1 GiB of HBM per device.

```python
import jax
import jax.numpy as jnp
from jax import lax

CZ = 128
CH = 128
N_RES = 384
ROW_BLOCK = 64
LAYERS = 2
LN_EPS = 1e-5


def setup_inputs(seed: int = 0, part: int = 0) -> dict:
    part_keys = jax.random.split(jax.random.fold_in(jax.random.key(seed), part), 2)
    shared_keys = jax.random.split(jax.random.key(seed + 1), 10)

    def draw_normal(key_index, shape, scale):
        return scale * jax.random.normal(shared_keys[key_index], shape, jnp.float32)

    pair_act = jax.random.normal(part_keys[0], (N_RES, N_RES, CZ), jnp.float32)
    mask_draw = jax.random.randint(part_keys[1], (N_RES, N_RES), 0, 10)
    pair_mask = (mask_draw >= 2).astype(jnp.int32)
    return {
        'pair_act': pair_act.astype(jnp.bfloat16),
        'pair_mask': pair_mask,
        'ln_in_scale': (1.0 + draw_normal(0, (LAYERS, CZ), 0.3)).astype(jnp.bfloat16),
        'ln_in_bias': draw_normal(1, (LAYERS, CZ), 0.3).astype(jnp.bfloat16),
        'w_in': draw_normal(2, (LAYERS, CZ, 4 * CH), CZ ** -0.5).astype(jnp.bfloat16),
        'b_in': draw_normal(3, (LAYERS, 4 * CH), 0.5).astype(jnp.bfloat16),
        'w_gate': draw_normal(4, (LAYERS, CZ, CZ), CZ ** -0.5).astype(jnp.bfloat16),
        'b_gate': draw_normal(5, (LAYERS, CZ), 0.5).astype(jnp.bfloat16),
        'ln_out_scale': (1.0 + draw_normal(6, (LAYERS, CH), 0.3)).astype(jnp.bfloat16),
        'ln_out_bias': draw_normal(7, (LAYERS, CH), 0.3).astype(jnp.bfloat16),
        'w_out': draw_normal(8, (LAYERS, CH, CZ), CH ** -0.5).astype(jnp.bfloat16),
        'b_out': draw_normal(9, (LAYERS, CZ), 0.3).astype(jnp.bfloat16),
    }


def layer_norm(values, ln_scale, offset):
    values = values.astype(jnp.float32)
    mean_val = jnp.mean(values, axis=-1, keepdims=True)
    centred = values - mean_val
    var_val = jnp.mean(centred * centred, axis=-1, keepdims=True)
    return centred * lax.rsqrt(var_val + LN_EPS) * ln_scale.astype(jnp.float32) + offset.astype(jnp.float32)


def gated_side(z_norm, mask_rows, w_pair, b_pair):
    projected = jnp.dot(z_norm.reshape(-1, CZ), w_pair, preferred_element_type=jnp.float32) + b_pair.astype(jnp.float32)
    gated = jax.nn.sigmoid(projected[:, CH:]) * projected[:, :CH] * mask_rows.reshape(-1, 1)
    return gated.astype(jnp.bfloat16).reshape(ROW_BLOCK, N_RES, CH)


def tri_update(z_cur, mask_f, layer_params):
    ln_in_s, ln_in_b, w_in_l, b_in_l, w_gate_l, b_gate_l, ln_out_s, ln_out_b, w_out_l, b_out_l = layer_params
    num_blocks = N_RES // ROW_BLOCK
    z_blocks = z_cur.reshape(num_blocks, ROW_BLOCK, N_RES, CZ)
    mask_blocks = mask_f.reshape(num_blocks, ROW_BLOCK, N_RES)

    def b_rows(block):
        z_rows, mask_rows = block
        z_norm = layer_norm(z_rows, ln_in_s, ln_in_b).astype(jnp.bfloat16)
        return gated_side(z_norm, mask_rows, w_in_l[:, 2 * CH:], b_in_l[2 * CH:])

    b_side = lax.map(b_rows, (z_blocks, mask_blocks)).reshape(N_RES, N_RES, CH).astype(jnp.float32)

    def out_rows(block):
        z_rows, mask_rows = block
        z_norm = layer_norm(z_rows, ln_in_s, ln_in_b).astype(jnp.bfloat16)
        a_side = gated_side(z_norm, mask_rows, w_in_l[:, :2 * CH], b_in_l[:2 * CH])
        tri_sum = jnp.einsum('ikc,jkc->ijc', a_side.astype(jnp.float32), b_side)
        o_norm = layer_norm(tri_sum, ln_out_s, ln_out_b).astype(jnp.bfloat16)
        update = jnp.dot(o_norm.reshape(-1, CH), w_out_l, preferred_element_type=jnp.float32) + b_out_l.astype(jnp.float32)
        update = update.astype(jnp.bfloat16).astype(jnp.float32)
        gate_val = jax.nn.sigmoid(jnp.dot(z_norm.reshape(-1, CZ), w_gate_l, preferred_element_type=jnp.float32) + b_gate_l.astype(jnp.float32))
        z_new = z_rows.reshape(-1, CZ).astype(jnp.float32) + gate_val * update
        return z_new.astype(jnp.bfloat16).reshape(ROW_BLOCK, N_RES, CZ)

    return lax.map(out_rows, (z_blocks, mask_blocks)).reshape(N_RES, N_RES, CZ)


def reference(pair_act, pair_mask, ln_in_scale, ln_in_bias, w_in, b_in, w_gate, b_gate, ln_out_scale, ln_out_bias, w_out, b_out):
    mask_f = pair_mask.astype(jnp.float32)

    def layer_step(z_cur, layer_params):
        return tri_update(z_cur, mask_f, layer_params), None

    stacked = (ln_in_scale, ln_in_bias, w_in, b_in, w_gate, b_gate, ln_out_scale, ln_out_bias, w_out, b_out)
    z_out, scan_tail = lax.scan(layer_step, pair_act, stacked)
    return z_out
```

```python
import functools
import jax
import jax.numpy as jnp
from jax import lax
from jax.experimental import pallas as pl
from jax.experimental.pallas import tpu as pltpu
from jax.sharding import PartitionSpec as P

LN_EPS = 1e-5
ROWS = 16
CHUNK = 16
PITCH = 136
NT = (((1,), (1,)), ((), ()))


def norm_lanes(x, scale, bias):
    mean = jnp.mean(x, axis=-1, keepdims=True)
    xc = x - mean
    var = jnp.mean(xc * xc, axis=-1, keepdims=True)
    return xc * lax.rsqrt(var + LN_EPS) * scale + bias


def project_kernel(sides, want_zn, *refs):
    z_refs, refs = refs[:4], refs[4:]
    mask_ref, w_ref, bias_ref, ln_s, ln_b = refs[:5]
    refs = refs[5:]
    outs, refs = refs[:sides], refs[sides:]
    zn_ref = None
    if want_zn:
        zn_ref, refs = refs[0], refs[1:]
    proj, stage = refs
    cols = z_refs[0].shape[2]

    def row(i, carry):
        parts = []
        for t in range(4):
            zn = norm_lanes(z_refs[t][i, 0].astype(jnp.float32), ln_s[...], ln_b[...]).astype(jnp.bfloat16)
            parts.append(zn)
            if want_zn:
                zn_ref[i, t] = zn
        zn = jnp.concatenate(parts, axis=0)
        proj[...] = lax.dot_general(w_ref[...], zn, NT, preferred_element_type=jnp.float32)
        base = pl.multiple_of(i * PITCH, 8)
        for lt in range(3):
            ls = slice(lt * 128, lt * 128 + 128)
            m = mask_ref[i, :, ls]
            for s in range(sides):
                value = proj[s * 256:s * 256 + 128, ls] + bias_ref[s * 256:s * 256 + 128]
                gate = proj[s * 256 + 128:s * 256 + 256, ls] + bias_ref[s * 256 + 128:s * 256 + 256]
                stage[s, lt, pl.ds(base, 128), :] = (jnp.tanh(gate) + 1.0) * value * m
        return carry

    lax.fori_loop(0, ROWS, row, 0)

    def chan(c, carry):
        for s in range(sides):
            for lt in range(3):
                outs[s][c, :, lt * 128:lt * 128 + 128] = stage[s, lt, pl.ds(c, ROWS, stride=PITCH), :].astype(jnp.bfloat16)
        return carry

    lax.fori_loop(0, 128, chan, 0, unroll=8)


def project(tiles, mask_f, w_t, bias, ln_s, ln_b, sides, want_zn):
    rows = tiles[0][0].shape[0]
    out_shape = [jax.ShapeDtypeStruct((128, rows, 384), jnp.bfloat16)] * sides
    out_specs = [pl.BlockSpec((128, ROWS, 384), lambda r: (0, r, 0))] * sides
    if want_zn:
        out_shape.append(jax.ShapeDtypeStruct((rows, 4, 96, 128), jnp.bfloat16))
        out_specs.append(pl.BlockSpec((ROWS, 4, 96, 128), lambda r: (r, 0, 0, 0)))
    full = lambda *shape: pl.BlockSpec(shape, lambda r: (0,) * len(shape))
    in_specs = [pl.BlockSpec((ROWS, 1, 96, 128), functools.partial(lambda b, r: (r, b, 0, 0), blk)) for _, blk in tiles]
    in_specs += [pl.BlockSpec((ROWS, 1, 384), lambda r: (r, 0, 0)), full(256 * sides, 128), full(256 * sides, 128), full(1, 128), full(1, 128)]
    return pl.pallas_call(
        functools.partial(project_kernel, sides, want_zn),
        grid=(rows // ROWS,),
        out_shape=out_shape,
        in_specs=in_specs,
        out_specs=out_specs,
        scratch_shapes=[pltpu.VMEM((256 * sides, 384), jnp.float32), pltpu.VMEM((sides, 3, ROWS * PITCH, 128), jnp.float32)],
        compiler_params=pltpu.CompilerParams(dimension_semantics=('arbitrary',), vmem_limit_bytes=48 * 2**20),
        cost_estimate=pl.CostEstimate(flops=rows * 384 * 128 * 512 * sides, bytes_accessed=rows * 384 * 256 * (2 + sides), transcendentals=0),
        name='project',
    )(*[arr for arr, _ in tiles], mask_f[:, None], w_t, bias, ln_s, ln_b)


def triangle_kernel(sets, group, where_ref, *refs):
    a_refs, refs = refs[:sets], refs[sets:]
    bm_ref, bo_ref = refs[:2]
    refs = refs[2:]
    z_refs, refs = refs[:sets], refs[sets:]
    zn_refs, refs = refs[:sets], refs[sets:]
    perm_ref, w_out, b_out, w_gate, b_gate, ln_s, ln_b = refs[:7]
    refs = refs[7:]
    outs, refs = refs[:sets], refs[sets:]
    tri, = refs
    step = pl.program_id(0)
    rows = a_refs[0].shape[1]

    def chan(cc, carry):
        a = jnp.concatenate([r[cc] for r in a_refs], axis=0)
        b = jnp.concatenate([bm_ref[cc], bo_ref[cc]], axis=0)
        o = lax.dot_general(a, b, NT, preferred_element_type=jnp.float32)
        tri[pl.ds(step * CHUNK + cc, sets * rows, stride=PITCH), :] = jnp.concatenate([o, o[:, :32]], axis=1)
        return carry

    lax.fori_loop(0, CHUNK, chan, 0, unroll=4)

    @pl.when(step == pl.num_programs(0) - 1)
    def _():
        for s in range(sets):
            def some(i, carry):
                i0 = i * group
                flipped = []
                for q in range(group):
                    o = tri[pl.ds(pl.multiple_of((s * rows + i0 + q) * PITCH, 8), 128), :]
                    mean = jnp.mean(o, axis=0, keepdims=True)
                    oc = o - mean
                    var = jnp.mean(oc * oc, axis=0, keepdims=True)
                    on = (oc * lax.rsqrt(var + LN_EPS) * ln_s[...] + ln_b[...]).astype(jnp.bfloat16)
                    flipped.append(lax.dot_general(perm_ref[...], on, NT, preferred_element_type=jnp.float32).astype(jnp.bfloat16))
                on = jnp.concatenate(flipped, axis=0)
                u = jnp.dot(on, w_out[...], preferred_element_type=jnp.float32) + b_out[...]
                u = u.astype(jnp.bfloat16).astype(jnp.float32)
                zn = jnp.concatenate([zn_refs[s][i0 + q, 0] for q in range(group)], axis=0)
                g = jnp.dot(zn, w_gate[...], preferred_element_type=jnp.float32) + b_gate[...]
                g = 0.5 * jnp.tanh(g) + 0.5
                for q in range(group):
                    sl = slice(q * 96, q * 96 + 96)
                    outs[s][i0 + q, 0] = (z_refs[s][i0 + q, 0].astype(jnp.float32) + g[sl] * u[sl]).astype(jnp.bfloat16)
                return carry
            lax.fori_loop(0, rows // group, some, 0)


def triangle(where, a_list, b_mine, b_other, z_list, zn_list, perm, w_out, b_out, w_gate, b_gate, ln_s, ln_b):
    sets = len(a_list)
    rows = a_list[0].shape[1]

    def tile_spec(rel):
        if rel is None:
            return pl.BlockSpec((rows, 1, 96, 128), lambda c, w: (0, 0, 0, 0))
        kind, rel = rel
        if kind == 'abs':
            return pl.BlockSpec((rows, 1, 96, 128), lambda c, w: (0, w[0] ^ rel, 0, 0))
        return pl.BlockSpec((rows, 1, 96, 128), lambda c, w: (0, rel, 0, 0))

    chan_spec = lambda r: pl.BlockSpec((CHUNK, r, 384), lambda c, w: (c, 0, 0))
    full = lambda *shape: pl.BlockSpec(shape, lambda c, w: (0,) * len(shape))
    out_spec = pl.BlockSpec((rows, 1, 96, 128), lambda c, w: (0, 0, 0, 0))
    in_specs = [chan_spec(rows)] * sets + [chan_spec(48)] * 2
    in_specs += [tile_spec(r) for _, r in z_list] + [tile_spec(r) for _, r in zn_list]
    in_specs += [full(96, 128), full(128, 128), full(1, 128), full(128, 128), full(1, 128), full(128, 128), full(128, 128)]
    return pl.pallas_call(
        functools.partial(triangle_kernel, sets, 4),
        out_shape=[jax.ShapeDtypeStruct((rows, 1, 96, 128), jnp.bfloat16)] * sets,
        grid_spec=pltpu.PrefetchScalarGridSpec(
            num_scalar_prefetch=1, grid=(128 // CHUNK,), in_specs=in_specs, out_specs=[out_spec] * sets,
            scratch_shapes=[pltpu.VMEM((sets * rows * PITCH, 128), jnp.float32)]),
        compiler_params=pltpu.CompilerParams(dimension_semantics=('arbitrary',), vmem_limit_bytes=48 * 2**20),
        cost_estimate=pl.CostEstimate(flops=sets * rows * 96 * 128 * 1800, bytes_accessed=(sets * rows + 96) * 384 * 256, transcendentals=0),
        name='triangle',
    )(where, *a_list, b_mine, b_other, *[z for z, _ in z_list], *[z for z, _ in zn_list], perm, w_out, b_out, w_gate, b_gate, ln_s, ln_b)


def solution(mesh):
    row_spec = P(('batch', 'dap'), None, None)
    mask_spec = P(('batch', 'dap'), None)
    vec_spec = P(None, None)
    mat_spec = P(None, None, None)

    def swap(x, bit):
        return lax.ppermute(x, 'dap', [(i, i ^ bit) for i in range(8)])

    def device_fn(z_rows, mask_rows, ln_in_scale, ln_in_bias, w_in, b_in, w_gate, b_gate, ln_out_scale, ln_out_bias, w_out, b_out):
        f32 = jnp.float32
        index = lax.axis_index('dap')
        chip, core = index // 2, index % 2
        z_own = z_rows.reshape(48, 4, 96, 128)
        z_x, z_y = swap(z_own, 2), swap(z_own, 4)
        mask_x, mask_y = swap(mask_rows, 2), swap(mask_rows, 4)
        masks = [m.astype(f32) for m in (mask_rows, mask_x, mask_y)]
        order = jnp.stack([chip ^ t for t in range(4)])
        masks_rel = [jnp.take(m.reshape(48, 4, 96), order, axis=1).reshape(48, 384) for m in masks]
        j = jnp.arange(96)
        source = jnp.where(core == 0, j, (j + 48) % 96)
        perm = (source[:, None] == jnp.arange(128)[None, :]).astype(jnp.bfloat16)
        zero = jnp.zeros((1,), jnp.int32)
        where = jnp.reshape(chip, (1,)).astype(jnp.int32)

        def lanes(v):
            return jnp.broadcast_to(v.astype(f32)[:, None], (v.shape[0], 128))

        def layer(l, tiles_o, tiles_x, tiles_y, mask3, wh, kind, last):
            half = jnp.bfloat16(0.5)
            w_t = w_in[l].T * half
            half_col = jnp.concatenate([jnp.full((256,), 0.5, f32)] * 2)
            bias = lanes(b_in[l].astype(f32) * half_col)
            ls, lb = ln_in_scale[l].astype(f32)[None], ln_in_bias[l].astype(f32)[None]
            a_o, b_o, zn_o = project(tiles_o, mask3[0], w_t, bias, ls, lb, 2, True)
            b_o2 = swap(b_o, 1)
            a_x, b_x, zn_x = project(tiles_x, mask3[1], w_t, bias, ls, lb, 2, True)
            b_x2 = swap(b_x, 1)
            b_y, = project(tiles_y, mask3[2], w_t[256:], bias[256:], ls, lb, 1, False)
            b_y2 = swap(b_y, 1)
            pieces = (perm, w_out[l], b_out[l].astype(f32)[None], w_gate[l] * half, b_gate[l].astype(f32)[None] * 0.5,
                      lanes(ln_out_scale[l]), lanes(ln_out_bias[l]))

            def run(sets, t, bm, bo):
                sel = {'o': (a_o, tiles_o[t], zn_o), 'x': (a_x, tiles_x[t], zn_x)}
                z_list = [(sel[s][1][0], (kind, t) if kind == 'abs' else None) for s in sets]
                return triangle(wh, [sel[s][0] for s in sets], bm, bo, z_list, [(sel[s][2], (kind, t)) for s in sets], *pieces)

            if not last:
                z_o0, z_x0 = run('ox', 0, b_o, b_o2)
                z_o1, z_x1 = run('ox', 1, b_x, b_x2)
                z_o2, z_x2 = run('ox', 2, b_y, b_y2)
                return (z_o0, z_o1, z_o2), (z_x0, z_x1, z_x2)
            z_o0, = run('o', 0, b_o, b_o2)
            z_o1, = run('o', 1, b_x, b_x2)
            z_o2, z_x2 = run('ox', 2, b_y, b_y2)
            return (z_o0, z_o1, z_o2), z_x2

        spread = lambda arr: [(arr, i) for i in range(4)]
        (o0, o1, o2), (x0, x1, x2) = layer(0, spread(z_own), spread(z_x), spread(z_y), masks, where, 'abs', False)
        x3, o3 = swap(o2, 2), swap(x2, 2)
        y2, y3, y0, y1 = swap(o0, 4), swap(o1, 4), swap(o2, 4), swap(o3, 4)
        tiles = lambda *arrs: [(arr, 0) for arr in arrs]
        (o0, o1, o2), x2 = layer(1, tiles(o0, o1, o2, o3), tiles(x0, x1, x2, x3), tiles(y0, y1, y2, y3), masks_rel, zero, 'rel', True)
        o3 = swap(x2, 2)
        out = jnp.zeros((48, 4, 96, 128), jnp.bfloat16)
        for t, tile in enumerate((o0, o1, o2, o3)):
            out = lax.dynamic_update_slice(out, tile, (0, chip ^ t, 0, 0))
        return out.reshape(48, 384, 128)

    return jax.shard_map(device_fn, mesh=mesh, in_specs=(row_spec, mask_spec, vec_spec, vec_spec, mat_spec, vec_spec, mat_spec, vec_spec, vec_spec, vec_spec, mat_spec, vec_spec), out_specs=row_spec, check_vma=False)
```

```python
import functools
import jax
import jax.numpy as jnp
from jax import lax
from jax.experimental import pallas as pl
from jax.experimental.pallas import tpu as pltpu
from jax.sharding import PartitionSpec as P

LN_EPS = 1e-5
ROWS = 16
CHUNK = 32
PITCH = 136
ROW_PITCH = 24
NT = (((1,), (1,)), ((), ()))


def norm_sublanes(x, scale, bias):
    mean = jnp.mean(x, axis=0, keepdims=True)
    xc = x - mean
    var = jnp.mean(xc * xc, axis=0, keepdims=True)
    return xc * lax.rsqrt(var + LN_EPS) * scale + bias


def project_kernel(sides, group, counts, *refs):
    sources, refs = [refs[5 * n:5 * n + 5] for n in range(len(counts))], refs[5 * len(counts):]
    bias_ref, centre, w_ref, ln_s, ln_b = refs[:5]
    outs = refs[6:6 + sides]
    proj, znt, stage = refs[6 + sides:]

    def block(z_refs, mask_ref):
        def normalise(i0):
            for h in range(group):
                z = jnp.concatenate([z_refs[t][i0 + h, 0] for t in range(4)], axis=0)
                xc = lax.dot_general(centre[...], z, NT, preferred_element_type=jnp.float32)
                for lt in range(3):
                    ls = slice(lt * 128, lt * 128 + 128)
                    x = xc[:, ls]
                    var = jnp.mean(x * x, axis=0, keepdims=True)
                    znt[h, :, ls] = (x * lax.rsqrt(var + LN_EPS) * ln_s[...] + ln_b[...]).astype(jnp.bfloat16)

        normalise(0)

        def some(g, carry):
            for h in range(group):
                proj[h] = jnp.dot(w_ref[...], znt[h], preferred_element_type=jnp.float32)
            normalise(jnp.minimum(g + 1, ROWS // group - 1) * group)
            for h in range(group):
                i = g * group + h
                for lt in range(3):
                    ls = slice(lt * 128, lt * 128 + 128)
                    m = mask_ref[i, :, ls]
                    for s in range(sides):
                        value = proj[h, s * 256:s * 256 + 128, ls] + bias_ref[s * 256:s * 256 + 128]
                        gate = proj[h, s * 256 + 128:s * 256 + 256, ls] + bias_ref[s * 256 + 128:s * 256 + 256]
                        stage[s, lt, pl.ds(i, 128, stride=ROW_PITCH), :] = (jnp.tanh(gate) + 1.0) * value * m
            return carry

        lax.fori_loop(0, ROWS // group, some, 0)

    if len(counts) == 1:
        block(sources[0][:4], sources[0][4])
    else:
        first = pl.program_id(0) < counts[0]
        pl.when(first)(lambda: block(sources[0][:4], sources[0][4]))
        pl.when(jnp.logical_not(first))(lambda: block(sources[1][:4], sources[1][4]))

    def chan(c, carry):
        for s in range(sides):
            for lt in range(3):
                outs[s][c, :, lt * 128:lt * 128 + 128] = stage[s, lt, pl.ds(pl.multiple_of(c * ROW_PITCH, 8), ROWS), :].astype(jnp.bfloat16)
        return carry

    lax.fori_loop(0, 128, chan, 0, unroll=8)


def project(sources, bias, w_t, ln_s, ln_b, centre, sides, dep, group=4):
    counts = [mask.shape[0] // ROWS for _, mask in sources]
    rows = sum(counts) * ROWS
    full = lambda *shape: pl.BlockSpec(shape, lambda r: (0,) * len(shape))
    in_specs, args, start = [], [], 0
    for (tiles, mask), count in zip(sources, counts):
        at = functools.partial(lambda lo, n, r: jnp.minimum(jnp.maximum(r - lo, 0), n - 1), start, count)
        for arr, blk in tiles:
            in_specs.append(pl.BlockSpec((ROWS, 1, 96, 128), functools.partial(lambda at, b, r: (at(r), b, 0, 0), at, blk)))
            args.append(arr)
        in_specs.append(pl.BlockSpec((ROWS, 1, 384), functools.partial(lambda at, r: (at(r), 0, 0), at)))
        args.append(mask)
        start += count
    in_specs += [full(256 * sides, 128), full(128, 128), full(256 * sides, 128), full(128, 128), full(128, 128), pl.BlockSpec(memory_space=pl.ANY)]
    return pl.pallas_call(
        functools.partial(project_kernel, sides, group, counts),
        grid=(rows // ROWS,),
        out_shape=[jax.ShapeDtypeStruct((128, rows, 384), jnp.bfloat16)] * sides,
        in_specs=in_specs,
        out_specs=[pl.BlockSpec((128, ROWS, 384), lambda r: (0, r, 0))] * sides,
        scratch_shapes=[pltpu.VMEM((group, 256 * sides, 384), jnp.float32), pltpu.VMEM((group, 128, 384), jnp.bfloat16), pltpu.VMEM((sides, 3, 128 * ROW_PITCH, 128), jnp.float32)],
        compiler_params=pltpu.CompilerParams(dimension_semantics=('arbitrary',), vmem_limit_bytes=62 * 2**20),
        cost_estimate=pl.CostEstimate(flops=rows * 384 * 128 * 512 * sides, bytes_accessed=rows * 384 * 256 * (1 + sides), transcendentals=0),
        name='project',
    )(*args, bias, centre, w_t, ln_s, ln_b, dep)


def triangle_kernel(sets, n_b, group, where_ref, *refs):
    pieces = [(s, n) for s, counts in enumerate(sets) for n in counts]
    a_refs, refs = refs[:len(pieces)], refs[len(pieces):]
    b_refs, refs = refs[:n_b], refs[n_b:]
    z_refs, refs = refs[:len(pieces)], refs[len(pieces):]
    perm_ref, w_out, b_out, w_gate, b_gate, ln_s, ln_b, in_s, in_b, centre = refs[:10]
    outs = refs[11:11 + len(sets)]
    tri, = refs[11 + len(sets):]
    step = pl.program_id(0)
    rows = sum(n for _, n in pieces)

    @pl.when(step == 0)
    def _():
        tri[:, 96:128] = jnp.zeros((rows * PITCH, 32), jnp.float32)

    def chan(cc, carry):
        a = jnp.concatenate([r[cc] for r in a_refs], axis=0)
        b = jnp.concatenate([r[cc] for r in b_refs], axis=0)
        tri[pl.ds(step * CHUNK + cc, rows, stride=PITCH), 0:96] = lax.dot_general(a, b, NT, preferred_element_type=jnp.float32)
        return carry

    lax.fori_loop(0, CHUNK, chan, 0, unroll=CHUNK)

    @pl.when(step == pl.num_programs(0) - 1)
    def _():
        row0 = 0
        done = [0] * len(sets)
        for k, (s, count) in enumerate(pieces):
            def some(i, carry, k=k, s=s, row0=row0, out0=done[s]):
                i0 = i * group
                flipped = []
                for q in range(group):
                    o = tri[pl.ds(pl.multiple_of((row0 + i0 + q) * PITCH, 8), 128), :]
                    on = norm_sublanes(o, ln_s[...], ln_b[...]).astype(jnp.bfloat16)
                    flipped.append(lax.dot_general(perm_ref[...], on, NT, preferred_element_type=jnp.float32).astype(jnp.bfloat16))
                on = jnp.concatenate(flipped, axis=0)
                u = jnp.dot(on, w_out[...], preferred_element_type=jnp.float32) + b_out[...]
                u = u.astype(jnp.bfloat16).astype(jnp.float32)
                zb = z_refs[k][pl.ds(i0, group), 0].reshape(group * 96, 128)
                xc = jnp.dot(zb, centre[...], preferred_element_type=jnp.float32)
                z = zb.astype(jnp.float32)
                var = jnp.mean(xc * xc, axis=-1, keepdims=True)
                zn = (xc * lax.rsqrt(var + LN_EPS) * in_s[...] + in_b[...]).astype(jnp.bfloat16)
                g = jnp.dot(zn, w_gate[...], preferred_element_type=jnp.float32) + b_gate[...]
                g = 0.5 * jnp.tanh(g) + 0.5
                outs[s][pl.ds(out0 + i0, group), 0] = (z + g * u).astype(jnp.bfloat16).reshape(group, 96, 128)
                return carry

            lax.fori_loop(0, count // group, some, 0)
            row0 += count
            done[s] += count


def triangle(where, sets, b_pieces, params, dep, into=None, group=16):
    flat = [p for pieces in sets for p in pieces]
    rows = sum(p[2] for p in flat)

    def tile_spec(n, rel):
        if rel is None:
            return pl.BlockSpec((n, 1, 96, 128), lambda c, w: (0, 0, 0, 0))
        return pl.BlockSpec((n, 1, 96, 128), lambda c, w: (0, w[0] ^ rel, 0, 0))

    chan_spec = lambda n, blk: pl.BlockSpec((CHUNK, n, 384), lambda c, w: (c, blk, 0))
    full = lambda *shape: pl.BlockSpec(shape, lambda c, w: (0,) * len(shape))
    in_specs = [chan_spec(p[2], p[1]) for p in flat] + [chan_spec(n, blk) for _, blk, n in b_pieces]
    in_specs += [tile_spec(p[2], p[4]) for p in flat]
    in_specs += [full(96, 128), full(128, 128), full(1, 128), full(128, 128), full(1, 128), full(128, 128), full(128, 128), full(1, 128), full(1, 128), full(128, 128)]
    in_specs.append(pl.BlockSpec(memory_space=pl.ANY))
    sizes = [[p[2] for p in pieces] for pieces in sets]
    width, out_rel, aliases = 1, None, {}
    if into is not None:
        width, out_rel = 4, into[1]
        if into[0] is not None:
            dep, aliases = into[0], {len(in_specs): 0}
    return pl.pallas_call(
        functools.partial(triangle_kernel, sizes, len(b_pieces), group),
        out_shape=[jax.ShapeDtypeStruct((sum(n), width, 96, 128), jnp.bfloat16) for n in sizes],
        input_output_aliases=aliases,
        grid_spec=pltpu.PrefetchScalarGridSpec(
            num_scalar_prefetch=1, grid=(128 // CHUNK,), in_specs=in_specs,
            out_specs=[tile_spec(sum(n), out_rel) for n in sizes],
            scratch_shapes=[pltpu.VMEM((rows * PITCH, 128), jnp.float32)]),
        compiler_params=pltpu.CompilerParams(dimension_semantics=('arbitrary',), vmem_limit_bytes=62 * 2**20),
        cost_estimate=pl.CostEstimate(flops=rows * 96 * 128 * 1800, bytes_accessed=(rows + 96) * 384 * 256, transcendentals=0),
        name='triangle',
    )(where, *[p[0] for p in flat], *[b for b, _, _ in b_pieces], *[p[3] for p in flat], *params, dep)


def solution(mesh):
    row_spec = P(('batch', 'dap'), None, None)
    mask_spec = P(('batch', 'dap'), None)
    vec_spec = P(None, None)
    mat_spec = P(None, None, None)

    def swap(x, bit):
        return lax.ppermute(x, 'dap', [(i, i ^ bit) for i in range(8)])

    def hold(x, *others):
        return lax.optimization_barrier((x,) + others)[0]

    def device_fn(z_rows, mask_rows, ln_in_scale, ln_in_bias, w_in, b_in, w_gate, b_gate, ln_out_scale, ln_out_bias, w_out, b_out):
        f32, bf16 = jnp.float32, jnp.bfloat16
        index = lax.axis_index('dap')
        chip, core = index // 2, index % 2
        z_own = z_rows.reshape(48, 4, 96, 128)
        z_xa, z_ya = swap(z_own[:32], 2), swap(z_own[:32], 4)
        z_xb, z_yb = swap(z_own[32:], 2), swap(z_own[32:], 4)
        mask_bf = mask_rows
        mask_x, mask_y = swap(mask_bf, 2), swap(mask_bf, 4)
        masks = [m.astype(f32)[:, None] for m in (mask_bf, mask_x, mask_y)]
        order = jnp.stack([chip ^ t for t in range(4)])
        masks_rel = [jnp.take(m.reshape(48, 1, 4, 96), order, axis=2).reshape(48, 1, 384) for m in masks]
        j = jnp.arange(96)
        source = jnp.where(core == 0, j, (j + 48) % 96)
        perm = (source[:, None] == jnp.arange(128)[None, :]).astype(bf16)
        eye = jnp.arange(128)[:, None] == jnp.arange(128)[None, :]
        centre = (eye.astype(f32) - 1.0 / 128).astype(bf16)
        zero = jnp.zeros((1,), jnp.int32)
        where = jnp.reshape(chip, (1,)).astype(jnp.int32)
        lanes = lambda v: jnp.broadcast_to(v.astype(f32)[:, None], (v.shape[0], 128))
        half = bf16(0.5)

        def weights(l):
            proj = (lanes(b_in[l].astype(f32) * 0.5), w_in[l].T * half, lanes(ln_in_scale[l]), lanes(ln_in_bias[l]), centre)
            tri = (perm, w_out[l], b_out[l].astype(f32)[None], w_gate[l] * half, b_gate[l].astype(f32)[None] * 0.5,
                   lanes(ln_out_scale[l]), lanes(ln_out_bias[l]), ln_in_scale[l].astype(f32)[None], ln_in_bias[l].astype(f32)[None], centre)
            return proj, tri

        (bias, w_t, ls, lb, ce), tri = weights(0)
        spread = lambda arr: [(arr, i) for i in range(4)]
        a_o, b_o = project([(spread(z_own), masks[0])], bias, w_t, ls, lb, ce, 2, perm)
        b_o2 = swap(b_o, 1)
        set_o = lambda t: [(a_o, 0, 48, z_own, t)]
        o0, = triangle(where, [set_o(0)], [(b_o, 0, 48), (b_o2, 0, 48)], tri, a_o)
        a_a, b_a = project([(spread(z_xa), masks[1][:32]), (spread(z_ya), masks[2][:32])], bias, w_t, ls, lb, ce, 2, o0)
        b_a2 = swap(b_a, 1)
        a_b, b_b = project([(spread(z_xb), masks[1][32:]), (spread(z_yb), masks[2][32:])], bias, w_t, ls, lb, ce, 2, a_a)
        b_b2 = swap(b_b, 1)
        o0s = hold(o0, z_xb, z_yb)
        x1, y2 = swap(o0s, 2), swap(o0s, 4)
        cols = lambda k: [(b_a, k, 32), (b_b, k, 16), (b_a2, k, 32), (b_b2, k, 16)]
        set_x = [(a_a, 0, 32, z_xa, 2), (a_b, 0, 16, z_xb, 2)]
        o2, x2 = triangle(where, [set_o(2), set_x], cols(1), tri, a_b)
        o3 = swap(x2, 2)
        o1, = triangle(where, [set_o(1)], cols(0), tri, o2)
        y3 = swap(o1, 4)
        set_x = [(a_a, 0, 32, z_xa, 0), (a_b, 0, 16, z_xb, 0)]
        set_y = [(a_a, 1, 32, z_ya, 0), (a_b, 1, 16, z_yb, 0)]
        x0, y0 = triangle(where, [set_x, set_y], [(b_o, 0, 48), (b_o2, 0, 48)], tri, o1)
        x3 = swap(o2, 2)
        y1 = swap(o3, 4)

        (bias, w_t, ls, lb, ce), tri = weights(1)
        tiles = lambda *arrs: [(arr, 0) for arr in arrs]
        a_o1, b_o1 = project([(tiles(o0, o1, o2, o3), masks_rel[0])], bias, w_t, ls, lb, ce, 2, x0)
        b_o12 = swap(b_o1, 1)
        set_o = lambda z: [(a_o1, 0, 48, z, None)]
        a_x1, b_x1 = project([(tiles(x0, x1, x2, x3), masks_rel[1])], bias, w_t, ls, lb, ce, 2, a_o1)
        b_x12 = swap(b_x1, 1)
        b_y1, = project([(tiles(y0, y1, y2, y3), masks_rel[2])], bias[256:], w_t[256:], ls, lb, ce, 1, a_x1)
        b_y12 = swap(b_y1, 1)
        out, = triangle(where, [set_o(o0)], [(b_o1, 0, 48), (b_o12, 0, 48)], tri, b_y1, (None, 0))
        q2, = triangle(where, [[(a_x1, 0, 48, x2, None)]], [(b_y1, 0, 48), (b_y12, 0, 48)], tri, out)
        p3 = swap(q2, 2)
        out, = triangle(where, [set_o(o2)], [(b_y1, 0, 48), (b_y12, 0, 48)], tri, q2, (out, 2))
        out, = triangle(where, [set_o(o1)], [(b_x1, 0, 48), (b_x12, 0, 48)], tri, q2, (out, 1))
        out = lax.dynamic_update_slice(out, p3, (0, chip ^ 3, 0, 0))
        return out.reshape(48, 384, 128)

    return jax.shard_map(device_fn, mesh=mesh, in_specs=(row_spec, mask_spec, vec_spec, vec_spec, mat_spec, vec_spec, mat_spec, vec_spec, vec_spec, vec_spec, mat_spec, vec_spec), out_specs=row_spec, check_vma=False)
```

```python
import functools
import jax
import jax.numpy as jnp
from jax import lax
from jax.experimental import pallas as pl
from jax.experimental.pallas import tpu as pltpu
from jax.sharding import PartitionSpec as P

LN_EPS = 1e-5
ROWS = 16
CHUNK = 32
PITCH = 136
ROW_PITCH = 20
NT = (((1,), (1,)), ((), ()))


def norm_sublanes(x, scale, bias):
    mean = jnp.mean(x, axis=0, keepdims=True)
    xc = x - mean
    var = jnp.mean(xc * xc, axis=0, keepdims=True)
    return xc * lax.rsqrt(var + LN_EPS) * scale + bias


def project_kernel(sides, group, counts, *refs):
    sources, refs = [refs[5 * n:5 * n + 5] for n in range(len(counts))], refs[5 * len(counts):]
    bias_ref, ln_s, ln_b, w_ref, centre = [r.at[0] for r in refs[:4]] + [refs[4]]
    outs = refs[6:6 + sides]
    proj, znt, stage, keep = refs[6 + sides:]

    def block(z_refs, mask_ref):
        for i in range(ROWS):
            keep[i] = mask_ref[i:i + 1].astype(jnp.float32)

        def normalise(i0):
            for h in range(group):
                z = jnp.concatenate([z_refs[t][i0 + h, 0] for t in range(4)], axis=0)
                xc = lax.dot_general(centre[...], z, NT, preferred_element_type=jnp.float32)
                for lt in range(3):
                    ls = slice(lt * 128, lt * 128 + 128)
                    x = xc[:, ls]
                    var = jnp.mean(x * x, axis=0, keepdims=True)
                    znt[h, :, ls] = (x * lax.rsqrt(var + LN_EPS) * ln_s[...] + ln_b[...]).astype(jnp.bfloat16)

        normalise(0)

        def some(g, carry):
            for h in range(group):
                proj[h] = jnp.dot(w_ref[...], znt[h], preferred_element_type=jnp.float32)
            normalise(jnp.minimum(g + 1, ROWS // group - 1) * group)
            for h in range(group):
                i = g * group + h
                for lt in range(3):
                    ls = slice(lt * 128, lt * 128 + 128)
                    m = keep[i, :, ls]
                    for s in range(sides):
                        value = proj[h, s * 256:s * 256 + 128, ls] + bias_ref[s * 256:s * 256 + 128]
                        gate = proj[h, s * 256 + 128:s * 256 + 256, ls] + bias_ref[s * 256 + 128:s * 256 + 256]
                        stage[s, lt, pl.ds(i, 128, stride=ROW_PITCH), :] = (jnp.tanh(gate) + 1.0) * value * m
            return carry

        lax.fori_loop(0, ROWS // group, some, 0)

    if len(counts) == 1:
        block(sources[0][:4], sources[0][4])
    else:
        first = pl.program_id(0) < counts[0]
        pl.when(first)(lambda: block(sources[0][:4], sources[0][4]))
        pl.when(jnp.logical_not(first))(lambda: block(sources[1][:4], sources[1][4]))

    def chan(c8, carry):
        for s in range(sides):
            for lt in range(3):
                view = stage.at[s, lt, pl.ds(pl.multiple_of(c8 * 8 * ROW_PITCH, 8), 8 * ROW_PITCH)]
                for q in range(8):
                    outs[s][c8 * 8 + q, :, lt * 128:lt * 128 + 128] = view[q * ROW_PITCH:q * ROW_PITCH + ROWS].astype(jnp.bfloat16)
        return carry

    lax.fori_loop(0, 16, chan, 0)


def project(layer, sources, vectors, w_t, centre, sides, dep, group=4):
    counts = [n // ROWS for n, _, _, _ in sources]
    rows = sum(counts) * ROWS
    in_specs, args, start = [], [], 0
    for (_, tiles, mask, mask_block), count in zip(sources, counts):
        at = functools.partial(lambda lo, n, r: jnp.minimum(jnp.maximum(r - lo, 0), n - 1), start, count)
        for arr, blk in tiles:
            in_specs.append(pl.BlockSpec((ROWS, 1, 96, 128), functools.partial(lambda at, b, r: (at(r), b, 0, 0), at, blk)))
            args.append(arr)
        in_specs.append(pl.BlockSpec((ROWS, 384), functools.partial(lambda at, b, r: (at(r) + b, 0), at, mask_block)))
        args.append(mask)
        start += count
    part = lambda n, blk: pl.BlockSpec((1, n, 128), lambda r: (layer, blk, 0))
    in_specs += [part(256 * sides, 2 - sides), part(128, 4), part(128, 5), part(256 * sides, 2 - sides), pl.BlockSpec((128, 128), lambda r: (0, 0)), pl.BlockSpec(memory_space=pl.ANY)]
    return pl.pallas_call(
        functools.partial(project_kernel, sides, group, counts),
        grid=(rows // ROWS,),
        out_shape=[jax.ShapeDtypeStruct((128, rows, 384), jnp.bfloat16)] * sides,
        in_specs=in_specs,
        out_specs=[pl.BlockSpec((128, ROWS, 384), lambda r: (0, r, 0))] * sides,
        scratch_shapes=[pltpu.VMEM((group, 256 * sides, 384), jnp.float32), pltpu.VMEM((group, 128, 384), jnp.bfloat16), pltpu.VMEM((sides, 3, 128 * ROW_PITCH, 128), jnp.float32), pltpu.VMEM((ROWS, 1, 384), jnp.float32)],
        compiler_params=pltpu.CompilerParams(dimension_semantics=('arbitrary',), vmem_limit_bytes=62 * 2**20),
        cost_estimate=pl.CostEstimate(flops=rows * 384 * 128 * 512 * sides, bytes_accessed=rows * 384 * 256 * (1 + sides), transcendentals=0),
        name='project',
    )(*args, vectors, vectors, vectors, w_t, centre, dep)


def triangle_kernel(sets, n_b, n_held, group, where_ref, *refs):
    pieces = [(s, n) for s, counts in enumerate(sets) for n in counts]
    a_refs, refs = refs[:len(pieces)], refs[len(pieces):]
    b_refs, refs = refs[:n_b], refs[n_b:]
    z_refs, refs = refs[:len(pieces)], refs[len(pieces):]
    perm_ref, centre = refs[:2]
    w_out, w_gate, ln_s, ln_b, rows_ref = [r.at[0] for r in refs[2:7]]
    b_out, b_gate, in_s, in_b = [rows_ref.at[n:n + 1] for n in range(4)]
    outs = refs[7 + n_held:7 + n_held + len(sets)]
    tri, = refs[7 + n_held + len(sets):]
    step = pl.program_id(0)
    rows = sum(n for _, n in pieces)

    @pl.when(step == 0)
    def _():
        tri[:, 96:128] = jnp.zeros((rows * PITCH, 32), jnp.float32)

    def chan(cc, carry):
        a = jnp.concatenate([r[cc] for r in a_refs], axis=0)
        b = jnp.concatenate([r[cc] for r in b_refs], axis=0)
        tri[pl.ds(step * CHUNK + cc, rows, stride=PITCH), 0:96] = lax.dot_general(a, b, NT, preferred_element_type=jnp.float32)
        return carry

    lax.fori_loop(0, CHUNK, chan, 0, unroll=CHUNK)

    @pl.when(step == pl.num_programs(0) - 1)
    def _():
        row0 = 0
        done = [0] * len(sets)
        for k, (s, count) in enumerate(pieces):
            def some(i, carry, k=k, s=s, row0=row0, out0=done[s]):
                i0 = i * group
                flipped = []
                for q in range(group):
                    o = tri[pl.ds(pl.multiple_of((row0 + i0 + q) * PITCH, 8), 128), :]
                    on = norm_sublanes(o, ln_s[...], ln_b[...]).astype(jnp.bfloat16)
                    flipped.append(lax.dot_general(perm_ref[...], on, NT, preferred_element_type=jnp.float32).astype(jnp.bfloat16))
                on = jnp.concatenate(flipped, axis=0)
                u = jnp.dot(on, w_out[...], preferred_element_type=jnp.float32) + b_out[...]
                u = u.astype(jnp.bfloat16).astype(jnp.float32)
                zb = z_refs[k][pl.ds(i0, group), 0].reshape(group * 96, 128)
                xc = jnp.dot(zb, centre[...], preferred_element_type=jnp.float32)
                z = zb.astype(jnp.float32)
                var = jnp.mean(xc * xc, axis=-1, keepdims=True)
                zn = (xc * lax.rsqrt(var + LN_EPS) * in_s[...] + in_b[...]).astype(jnp.bfloat16)
                g = jnp.dot(zn, w_gate[...], preferred_element_type=jnp.float32) + b_gate[...]
                g = 0.5 * jnp.tanh(g) + 0.5
                outs[s][pl.ds(out0 + i0, group), 0] = (z + g * u).astype(jnp.bfloat16).reshape(group, 96, 128)
                return carry

            lax.fori_loop(0, count // group, some, 0)
            row0 += count
            done[s] += count


def triangle(layer, where, sets, b_pieces, params, dep, into=None, group=16):
    flat = [p for pieces in sets for p in pieces]
    rows = sum(p[2] for p in flat)

    def tile_spec(n, rel):
        if rel is None:
            return pl.BlockSpec((n, 1, 96, 128), lambda c, w: (0, 0, 0, 0))
        return pl.BlockSpec((n, 1, 96, 128), lambda c, w: (0, w[0] ^ rel, 0, 0))

    chan_spec = lambda n, blk: pl.BlockSpec((CHUNK, n, 384), lambda c, w: (c, blk, 0))
    full = lambda *shape: pl.BlockSpec(shape, lambda c, w: (0,) * len(shape))
    in_specs = [chan_spec(p[2], p[1]) for p in flat] + [chan_spec(n, blk) for _, blk, n in b_pieces]
    in_specs += [tile_spec(p[2], p[4]) for p in flat]
    part = lambda n, blk: pl.BlockSpec((1, n, 128), lambda c, w: (layer, blk, 0))
    in_specs += [full(96, 128), full(128, 128), part(128, 0), part(128, 0), part(128, 6), part(128, 7), part(4, 0)]
    sizes = [[p[2] for p in pieces] for pieces in sets]
    into = into or [(n, 1, 0, None, None) for n in map(sum, sizes)]
    deps = dep if isinstance(dep, tuple) else (dep,)
    in_specs += [pl.BlockSpec(memory_space=pl.ANY)] * len(deps)
    aliases, held = {}, []
    for s, (_, _, _, _, prev) in enumerate(into):
        if prev is not None:
            aliases[1 + len(in_specs) + len(held)] = s
            held.append(prev)
    in_specs += [pl.BlockSpec(memory_space=pl.ANY)] * len(held)

    def out_spec(n, blk, rel):
        if rel is None:
            return pl.BlockSpec((n, 1, 96, 128), lambda c, w: (blk, 0, 0, 0))
        return pl.BlockSpec((n, 1, 96, 128), lambda c, w: (blk, w[0] ^ rel, 0, 0))

    return pl.pallas_call(
        functools.partial(triangle_kernel, sizes, len(b_pieces), len(deps) + len(held), group),
        out_shape=[jax.ShapeDtypeStruct((total, width, 96, 128), jnp.bfloat16) for total, width, _, _, _ in into],
        input_output_aliases=aliases,
        grid_spec=pltpu.PrefetchScalarGridSpec(
            num_scalar_prefetch=1, grid=(128 // CHUNK,), in_specs=in_specs,
            out_specs=[out_spec(sum(n), blk, rel) for n, (_, _, blk, rel, _) in zip(sizes, into)],
            scratch_shapes=[pltpu.VMEM((rows * PITCH, 128), jnp.float32)]),
        compiler_params=pltpu.CompilerParams(dimension_semantics=('arbitrary',), vmem_limit_bytes=62 * 2**20),
        cost_estimate=pl.CostEstimate(flops=rows * 96 * 128 * 1800, bytes_accessed=(rows + 96) * 384 * 256, transcendentals=0),
        name='triangle',
    )(where, *[p[0] for p in flat], *[b for b, _, _ in b_pieces], *[p[3] for p in flat], *params, *deps, *held)


def solution(mesh):
    row_spec = P(('batch', 'dap'), None, None)
    mask_spec = P(('batch', 'dap'), None)
    vec_spec = P(None, None)
    mat_spec = P(None, None, None)

    def swap(x, bit):
        return lax.ppermute(x, 'dap', [(i, i ^ bit) for i in range(8)])

    def hold(x, *others):
        return lax.optimization_barrier((x,) + others)[0]

    def device_fn(z_rows, mask_rows, ln_in_scale, ln_in_bias, w_in, b_in, w_gate, b_gate, ln_out_scale, ln_out_bias, w_out, b_out):
        f32, bf16 = jnp.float32, jnp.bfloat16
        index = lax.axis_index('dap')
        chip, core = index // 2, index % 2
        z_own = z_rows.reshape(48, 4, 96, 128)
        z_x, z_y = [], []
        for n in range(3):
            part = (z_own if n == 0 else lax.optimization_barrier(z_own))[16 * n:16 * n + 16]
            z_x.append(swap(part, 2))
            z_y.append(swap(part, 4))
        mask_bf = mask_rows
        mask_x, mask_y = swap(mask_bf, 2), swap(mask_bf, 4)
        masks = [mask_bf, mask_x, mask_y]
        cut = lambda m, n: [m[:, i * n:i * n + n] for i in range(384 // n)]
        rel = jnp.concatenate(masks, axis=0)
        h = cut(rel, 192)
        rel = jnp.where(chip >= 2, jnp.concatenate([h[1], h[0]], axis=1), rel)
        q = cut(rel, 96)
        rel = jnp.where(chip % 2 == 1, jnp.concatenate([q[1], q[0], q[3], q[2]], axis=1), rel)
        j = jnp.arange(96)
        source = jnp.where(core == 0, j, (j + 48) % 96)
        perm = (source[:, None] == jnp.arange(128)[None, :]).astype(bf16)
        eye = jnp.arange(128)[:, None] == jnp.arange(128)[None, :]
        centre = (eye.astype(f32) - 1.0 / 128).astype(bf16)
        zero = jnp.zeros((1,), jnp.int32)
        where = jnp.reshape(chip, (1,)).astype(jnp.int32)
        vectors = jnp.concatenate([b_in.astype(f32) * 0.5] + [v.astype(f32) for v in (ln_in_scale, ln_in_bias, ln_out_scale, ln_out_bias)], axis=1)
        vectors = jnp.broadcast_to(vectors[:, :, None], (2, 1024, 128))
        rows4 = jnp.stack([b_out.astype(f32), b_gate.astype(f32) * 0.5, ln_in_scale.astype(f32), ln_in_bias.astype(f32)], axis=1)
        w_t = jnp.swapaxes(w_in * bf16(0.5), 1, 2)
        tri = (perm, centre, w_out, w_gate * bf16(0.5), vectors, vectors, rows4)
        spread = lambda arr: [(arr, i) for i in range(4)]
        a_o, b_o = project(0, [(48, spread(z_own), mask_bf, 0)], vectors, w_t, centre, 2, perm)
        b_o2 = swap(b_o, 1)
        set_o = lambda t: [(a_o, 0, 48, z_own, t)]
        o0, = triangle(0, where, [set_o(0)], [(b_o, 0, 48), (b_o2, 0, 48)], tri, a_o)
        parts, last = [], o0
        for n in range(3):
            if n == 2:
                pair = lambda m, rel: ([(parts[m][0], 0, 16, z_x[m], rel)], [(parts[m][0], 1, 16, z_y[m], rel)])
                (xa, ya), (xb, yb) = pair(0, 0), pair(1, 0)
                x0, y0 = triangle(0, where, [xa + xb, ya + yb], [(b_o, 0, 48), (b_o2, 0, 48)], tri, (last, rel), [(48, 1, 0, None, None)] * 2)
                last = x0
            a_n, b_n = project(0, [(16, spread(z_x[n]), mask_x, n), (16, spread(z_y[n]), mask_y, n)], vectors, w_t, centre, 2, last)
            parts.append((a_n, b_n, swap(b_n, 1)))
            last = a_n
        o0s = hold(o0, z_x[2], z_y[2])
        x1, y2 = swap(o0s, 2), swap(o0s, 4)
        cols = lambda k: [(p[1], k, 16) for p in parts] + [(p[2], k, 16) for p in parts]
        set_x = [(parts[n][0], 0, 16, z_x[n], 2) for n in range(3)]
        o2, x2 = triangle(0, where, [set_o(2), set_x], cols(1), tri, last)
        o3 = swap(x2, 2)
        x3 = swap(o2, 2)
        o1, = triangle(0, where, [set_o(1)], cols(0), tri, o2)
        y3 = swap(o1, 4)
        y1 = swap(o3, 4)
        xc, yc = pair(2, 0)
        x0, y0 = triangle(0, where, [xc, yc], [(b_o, 0, 48), (b_o2, 0, 48)], tri, o1, [(48, 1, 2, None, x0), (48, 1, 2, None, y0)])

        tiles = lambda *arrs: [(arr, 0) for arr in arrs]
        a_o1, b_o1 = project(1, [(48, tiles(o0, o1, o2, o3), rel, 0)], vectors, w_t, centre, 2, x0)
        b_o12 = swap(b_o1, 1)
        set_o = lambda z: [(a_o1, 0, 48, z, None)]
        a_x1, b_x1 = project(1, [(48, tiles(x0, x1, x2, x3), rel, 3)], vectors, w_t, centre, 2, a_o1)
        b_x12 = swap(b_x1, 1)
        b_y1, = project(1, [(48, tiles(y0, y1, y2, y3), rel, 6)], vectors, w_t, centre, 1, a_x1)
        b_y12 = swap(b_y1, 1)
        out, = triangle(1, where, [set_o(o0)], [(b_o1, 0, 48), (b_o12, 0, 48)], tri, b_y1, [(48, 4, 0, 0, None)])
        q2, = triangle(1, where, [[(a_x1, 0, 48, x2, None)]], [(b_y1, 0, 48), (b_y12, 0, 48)], tri, out)
        p3 = swap(q2, 2)
        out, = triangle(1, where, [set_o(o2)], [(b_y1, 0, 48), (b_y12, 0, 48)], tri, q2, [(48, 4, 0, 2, out)])
        out, = triangle(1, where, [set_o(o1)], [(b_x1, 0, 48), (b_x12, 0, 48)], tri, q2, [(48, 4, 0, 1, out)])
        out = lax.dynamic_update_slice(out, p3, (0, chip ^ 3, 0, 0))
        return out.reshape(48, 384, 128)

    return jax.shard_map(device_fn, mesh=mesh, in_specs=(row_spec, mask_spec, vec_spec, vec_spec, mat_spec, vec_spec, mat_spec, vec_spec, vec_spec, vec_spec, mat_spec, vec_spec), out_specs=row_spec, check_vma=False)
```

```python
import functools
import jax
import jax.numpy as jnp
from jax import lax
from jax.experimental import pallas as pl
from jax.experimental.pallas import tpu as pltpu
from jax.sharding import PartitionSpec as P

LN_EPS = 1e-5
ROWS = 16
CHUNK = 16
GROUP = 16
PITCH = 136
ROW_PITCH = 20
NT = (((1,), (1,)), ((), ()))


def norm_sublanes(x, scale, bias):
    mean = jnp.mean(x, axis=0, keepdims=True)
    xc = x - mean
    var = jnp.mean(xc * xc, axis=0, keepdims=True)
    return xc * lax.rsqrt(var + LN_EPS) * scale + bias


def project_kernel(sides, group, counts, *refs):
    sources, refs = [refs[5 * n:5 * n + 5] for n in range(len(counts))], refs[5 * len(counts):]
    bias_ref, ln_s, ln_b, w_ref, centre = [r.at[0] for r in refs[:4]] + [refs[4]]
    outs = refs[6:6 + sides]
    proj, znt, stage, keep = refs[6 + sides:]

    def block(z_refs, mask_ref):
        for i in range(ROWS):
            keep[i] = mask_ref[i:i + 1].astype(jnp.float32)

        def normalise(i0):
            for h in range(group):
                z = jnp.concatenate([z_refs[t][i0 + h, 0] for t in range(4)], axis=0)
                xc = lax.dot_general(centre[...], z, NT, preferred_element_type=jnp.float32)
                for lt in range(3):
                    ls = slice(lt * 128, lt * 128 + 128)
                    x = xc[:, ls]
                    var = jnp.mean(x * x, axis=0, keepdims=True)
                    znt[h, :, ls] = (x * lax.rsqrt(var + LN_EPS) * ln_s[...] + ln_b[...]).astype(jnp.bfloat16)

        normalise(0)

        def some(g, carry):
            for h in range(group):
                proj[h] = jnp.dot(w_ref[...], znt[h], preferred_element_type=jnp.float32)
            normalise(jnp.minimum(g + 1, ROWS // group - 1) * group)
            for h in range(group):
                i = g * group + h
                for lt in range(3):
                    ls = slice(lt * 128, lt * 128 + 128)
                    m = keep[i, :, ls]
                    for s in range(sides):
                        value = proj[h, s * 256:s * 256 + 128, ls] + bias_ref[s * 256:s * 256 + 128]
                        gate = proj[h, s * 256 + 128:s * 256 + 256, ls] + bias_ref[s * 256 + 128:s * 256 + 256]
                        stage[s, lt, pl.ds(i, 128, stride=ROW_PITCH), :] = (jnp.tanh(gate) + 1.0) * value * m
            return carry

        lax.fori_loop(0, ROWS // group, some, 0)

    if len(counts) == 1:
        block(sources[0][:4], sources[0][4])
    else:
        first = pl.program_id(0) < counts[0]
        pl.when(first)(lambda: block(sources[0][:4], sources[0][4]))
        pl.when(jnp.logical_not(first))(lambda: block(sources[1][:4], sources[1][4]))

    def chan(c8, carry):
        for s in range(sides):
            for lt in range(3):
                view = stage.at[s, lt, pl.ds(pl.multiple_of(c8 * 8 * ROW_PITCH, 8), 8 * ROW_PITCH)]
                for q in range(8):
                    outs[s][c8 * 8 + q, :, lt * 128:lt * 128 + 128] = view[q * ROW_PITCH:q * ROW_PITCH + ROWS].astype(jnp.bfloat16)
        return carry

    lax.fori_loop(0, 16, chan, 0)


def project(layer, sources, vectors, w_t, centre, sides, dep, group=4):
    counts = [n // ROWS for n, _, _, _ in sources]
    rows = sum(counts) * ROWS
    in_specs, args, start = [], [], 0
    for (_, tiles, mask, mask_block), count in zip(sources, counts):
        at = functools.partial(lambda lo, n, r: jnp.minimum(jnp.maximum(r - lo, 0), n - 1), start, count)
        for arr, blk in tiles:
            in_specs.append(pl.BlockSpec((ROWS, 1, 96, 128), functools.partial(lambda at, b, r: (at(r), b, 0, 0), at, blk)))
            args.append(arr)
        in_specs.append(pl.BlockSpec((ROWS, 384), functools.partial(lambda at, b, r: (at(r) + b, 0), at, mask_block)))
        args.append(mask)
        start += count
    part = lambda n, blk: pl.BlockSpec((1, n, 128), lambda r: (layer, blk, 0))
    in_specs += [part(256 * sides, 2 - sides), part(128, 4), part(128, 5), part(256 * sides, 2 - sides), pl.BlockSpec((128, 128), lambda r: (0, 0)), pl.BlockSpec(memory_space=pl.ANY)]
    return pl.pallas_call(
        functools.partial(project_kernel, sides, group, counts),
        grid=(rows // ROWS,),
        out_shape=[jax.ShapeDtypeStruct((128, rows, 384), jnp.bfloat16)] * sides,
        in_specs=in_specs,
        out_specs=[pl.BlockSpec((128, ROWS, 384), lambda r: (0, r, 0))] * sides,
        scratch_shapes=[pltpu.VMEM((group, 256 * sides, 384), jnp.float32), pltpu.VMEM((group, 128, 384), jnp.bfloat16), pltpu.VMEM((sides, 3, 128 * ROW_PITCH, 128), jnp.float32), pltpu.VMEM((ROWS, 1, 384), jnp.float32)],
        compiler_params=pltpu.CompilerParams(dimension_semantics=('arbitrary',), vmem_limit_bytes=62 * 2**20),
        cost_estimate=pl.CostEstimate(flops=rows * 384 * 128 * 512 * sides, bytes_accessed=rows * 384 * 256 * (1 + sides), transcendentals=0),
        name='project',
    )(*args, vectors, vectors, vectors, w_t, centre, dep)


def triangle_kernel(pieces, b_pieces, out_at, n_held, where_ref, *refs):
    n_a, n_b = len(pieces), len(b_pieces)
    a_refs, refs = refs[:n_a], refs[n_a:]
    b_refs, refs = refs[:n_b], refs[n_b:]
    z_refs, refs = refs[:n_a], refs[n_a:]
    perm_ref, centre = refs[:2]
    w_out, w_gate, ln_s, ln_b, rows_ref = [r.at[0] for r in refs[2:7]]
    b_out, b_gate, in_s, in_b = [rows_ref.at[n:n + 1] for n in range(4)]
    outs, refs = refs[7 + n_held:7 + n_held + len(out_at)], refs[7 + n_held + len(out_at):]
    tri, abuf, bbuf, zbuf, obuf, load_sem, z_sem, out_sem = refs
    rows = sum(p[2] for p in pieces)
    column = lambda rel: 0 if rel is None else where_ref[0] ^ rel

    def loads(q):
        chans = pl.ds(pl.multiple_of(q * CHUNK, CHUNK), CHUNK)
        copies, r0 = [], 0
        for n, (_, blk, count, _) in enumerate(pieces):
            copies.append(pltpu.make_async_copy(a_refs[n].at[chans, blk * count:blk * count + count], abuf.at[chans, r0:r0 + count], load_sem.at[q, n]))
            r0 += count
        r0 = 0
        for n, (blk, count) in enumerate(b_pieces):
            copies.append(pltpu.make_async_copy(b_refs[n].at[chans, blk * count:blk * count + count], bbuf.at[chans, r0:r0 + count], load_sem.at[q, n_a + n]))
            r0 += count
        return copies

    def z_loads():
        copies, r0 = [], 0
        for n, (_, _, count, rel) in enumerate(pieces):
            copies.append(pltpu.make_async_copy(z_refs[n].at[:, column(rel)], zbuf.at[r0:r0 + count], z_sem.at[n]))
            r0 += count
        return copies

    def start_loads(q, carry):
        for copy in loads(q):
            copy.start()
        return carry

    lax.fori_loop(0, 128 // CHUNK, start_loads, 0)
    for copy in z_loads():
        copy.start()
    tri[:, 96:128] = jnp.zeros((rows * PITCH, 32), jnp.float32)

    def some_channels(q, carry):
        for copy in loads(q):
            copy.wait()
        for cc in range(CHUNK):
            c = q * CHUNK + cc
            tri[pl.ds(c, rows, stride=PITCH), 0:96] = lax.dot_general(abuf[c], bbuf[c], NT, preferred_element_type=jnp.float32)
        return carry

    lax.fori_loop(0, 128 // CHUNK, some_channels, 0)
    for copy in z_loads():
        copy.wait()

    def some_rows(i0):
        flipped = []
        for q in range(GROUP):
            o = tri[pl.ds(pl.multiple_of((i0 + q) * PITCH, 8), 128), :]
            on = norm_sublanes(o, ln_s[...], ln_b[...]).astype(jnp.bfloat16)
            flipped.append(lax.dot_general(perm_ref[...], on, NT, preferred_element_type=jnp.float32).astype(jnp.bfloat16))
        on = jnp.concatenate(flipped, axis=0)
        u = jnp.dot(on, w_out[...], preferred_element_type=jnp.float32) + b_out[...]
        u = u.astype(jnp.bfloat16).astype(jnp.float32)
        zb = zbuf[pl.ds(i0, GROUP)].reshape(GROUP * 96, 128)
        xc = jnp.dot(zb, centre[...], preferred_element_type=jnp.float32)
        z = zb.astype(jnp.float32)
        var = jnp.mean(xc * xc, axis=-1, keepdims=True)
        zn = (xc * lax.rsqrt(var + LN_EPS) * in_s[...] + in_b[...]).astype(jnp.bfloat16)
        g = jnp.dot(zn, w_gate[...], preferred_element_type=jnp.float32) + b_gate[...]
        g = 0.5 * jnp.tanh(g) + 0.5
        obuf[pl.ds(i0, GROUP)] = (z + g * u).astype(jnp.bfloat16).reshape(GROUP, 96, 128)

    spans, r0, done = [], 0, [at for at, _ in out_at]
    for s, _, count, _ in pieces:
        if spans and spans[-1][0] == s:
            spans[-1][2] += count
        else:
            spans.append([s, r0, count, done[s]])
        done[s] += count
        r0 += count

    def store(s, r0, at, i):
        row, to = pl.multiple_of(r0 + i * GROUP, GROUP), pl.multiple_of(at + i * GROUP, GROUP)
        return pltpu.make_async_copy(obuf.at[pl.ds(row, GROUP)], outs[s].at[pl.ds(to, GROUP), column(out_at[s][1])], out_sem.at[(r0 // GROUP) + i])

    for s, r0, count, at in spans:
        def body(i, carry, s=s, r0=r0, at=at):
            some_rows(pl.multiple_of(r0 + i * GROUP, GROUP))
            store(s, r0, at, i).start()
            return carry

        lax.fori_loop(0, count // GROUP, body, 0)
    for s, r0, count, at in spans:
        for i in range(count // GROUP):
            store(s, r0, at, i).wait()


def triangle(layer, where, sets, b_pieces, params, dep, into=None):
    flat = [(s,) + p for s, pieces in enumerate(sets) for p in pieces]
    rows = sum(p[3] for p in flat)
    into = into or [(sum(p[2] for p in pieces), 1, 0, None, None) for pieces in sets]
    deps = dep if isinstance(dep, tuple) else (dep,)
    held = [prev for _, _, _, _, prev in into if prev is not None]
    first = 1 + 2 * len(flat) + len(b_pieces) + 7 + len(deps)
    aliases, seen = {}, 0
    for s, (_, _, _, _, prev) in enumerate(into):
        if prev is not None:
            aliases[first + seen] = s
            seen += 1
    anywhere = pl.BlockSpec(memory_space=pl.ANY)
    full = lambda *shape: pl.BlockSpec(shape, lambda c, w: (0,) * len(shape))
    part = lambda n, blk: pl.BlockSpec((1, n, 128), lambda c, w: (layer, blk, 0))
    in_specs = [anywhere] * (2 * len(flat) + len(b_pieces))
    in_specs += [full(96, 128), full(128, 128), part(128, 0), part(128, 0), part(128, 6), part(128, 7), part(4, 0)]
    in_specs += [anywhere] * (len(deps) + len(held))
    return pl.pallas_call(
        functools.partial(triangle_kernel, [(p[0], p[2], p[3], p[5]) for p in flat], [(blk, n) for _, blk, n in b_pieces],
                          [(at, rel) for _, _, at, rel, _ in into], len(deps) + len(held)),
        out_shape=[jax.ShapeDtypeStruct((total, width, 96, 128), jnp.bfloat16) for total, width, _, _, _ in into],
        input_output_aliases=aliases,
        grid_spec=pltpu.PrefetchScalarGridSpec(
            num_scalar_prefetch=1, grid=(1,), in_specs=in_specs, out_specs=[anywhere] * len(into),
            scratch_shapes=[pltpu.VMEM((rows * PITCH, 128), jnp.float32), pltpu.VMEM((128, rows, 384), jnp.bfloat16), pltpu.VMEM((128, 96, 384), jnp.bfloat16),
                            pltpu.VMEM((rows, 96, 128), jnp.bfloat16), pltpu.VMEM((rows, 96, 128), jnp.bfloat16),
                            pltpu.SemaphoreType.DMA((128 // CHUNK, len(flat) + len(b_pieces))), pltpu.SemaphoreType.DMA((len(flat),)), pltpu.SemaphoreType.DMA((rows // GROUP,))]),
        compiler_params=pltpu.CompilerParams(dimension_semantics=('arbitrary',), vmem_limit_bytes=62 * 2**20),
        cost_estimate=pl.CostEstimate(flops=rows * 96 * 128 * 1800, bytes_accessed=(rows + 96) * 384 * 256, transcendentals=0),
        name='triangle',
    )(where, *[p[1] for p in flat], *[b for b, _, _ in b_pieces], *[p[4] for p in flat], *params, *deps, *held)


def solution(mesh):
    row_spec = P(('batch', 'dap'), None, None)
    mask_spec = P(('batch', 'dap'), None)
    vec_spec = P(None, None)
    mat_spec = P(None, None, None)

    def swap(x, bit):
        return lax.ppermute(x, 'dap', [(i, i ^ bit) for i in range(8)])

    def hold(x, *others):
        return lax.optimization_barrier((x,) + others)[0]

    def device_fn(z_rows, mask_rows, ln_in_scale, ln_in_bias, w_in, b_in, w_gate, b_gate, ln_out_scale, ln_out_bias, w_out, b_out):
        f32, bf16 = jnp.float32, jnp.bfloat16
        index = lax.axis_index('dap')
        chip, core = index // 2, index % 2
        z_own = z_rows.reshape(48, 4, 96, 128)
        z_x, z_y = [], []
        for n in range(3):
            part = (z_own if n == 0 else lax.optimization_barrier(z_own))[16 * n:16 * n + 16]
            z_x.append(swap(part, 2))
            z_y.append(swap(part, 4))
        mask_bf = mask_rows
        mask_x, mask_y = swap(mask_bf, 2), swap(mask_bf, 4)
        masks = [mask_bf, mask_x, mask_y]
        cut = lambda m, n: [m[:, i * n:i * n + n] for i in range(384 // n)]
        rel = jnp.concatenate(masks, axis=0)
        h = cut(rel, 192)
        rel = jnp.where(chip >= 2, jnp.concatenate([h[1], h[0]], axis=1), rel)
        q = cut(rel, 96)
        rel = jnp.where(chip % 2 == 1, jnp.concatenate([q[1], q[0], q[3], q[2]], axis=1), rel)
        j = jnp.arange(96)
        source = jnp.where(core == 0, j, (j + 48) % 96)
        perm = (source[:, None] == jnp.arange(128)[None, :]).astype(bf16)
        eye = jnp.arange(128)[:, None] == jnp.arange(128)[None, :]
        centre = (eye.astype(f32) - 1.0 / 128).astype(bf16)
        zero = jnp.zeros((1,), jnp.int32)
        where = jnp.reshape(chip, (1,)).astype(jnp.int32)
        vectors = jnp.concatenate([b_in.astype(f32) * 0.5] + [v.astype(f32) for v in (ln_in_scale, ln_in_bias, ln_out_scale, ln_out_bias)], axis=1)
        vectors = jnp.broadcast_to(vectors[:, :, None], (2, 1024, 128))
        rows4 = jnp.stack([b_out.astype(f32), b_gate.astype(f32) * 0.5, ln_in_scale.astype(f32), ln_in_bias.astype(f32)], axis=1)
        w_t = jnp.swapaxes(w_in * bf16(0.5), 1, 2)
        tri = (perm, centre, w_out, w_gate * bf16(0.5), vectors, vectors, rows4)
        spread = lambda arr: [(arr, i) for i in range(4)]
        a_o, b_o = project(0, [(48, spread(z_own), mask_bf, 0)], vectors, w_t, centre, 2, perm)
        b_o2 = swap(b_o, 1)
        set_o = lambda t: [(a_o, 0, 48, z_own, t)]
        o0, = triangle(0, where, [set_o(0)], [(b_o, 0, 48), (b_o2, 0, 48)], tri, a_o)
        parts, last = [], o0
        for n in range(3):
            if n == 2:
                pair = lambda m, rel: ([(parts[m][0], 0, 16, z_x[m], rel)], [(parts[m][0], 1, 16, z_y[m], rel)])
                (xa, ya), (xb, yb) = pair(0, 0), pair(1, 0)
                x0, y0 = triangle(0, where, [xa + xb, ya + yb], [(b_o, 0, 48), (b_o2, 0, 48)], tri, (last, rel), [(48, 1, 0, None, None)] * 2)
                last = x0
            a_n, b_n = project(0, [(16, spread(z_x[n]), mask_x, n), (16, spread(z_y[n]), mask_y, n)], vectors, w_t, centre, 2, last)
            parts.append((a_n, b_n, swap(b_n, 1)))
            last = a_n
        o0s = hold(o0, z_x[2], z_y[2])
        x1, y2 = swap(o0s, 2), swap(o0s, 4)
        cols = lambda k: [(p[1], k, 16) for p in parts] + [(p[2], k, 16) for p in parts]
        set_x = [(parts[n][0], 0, 16, z_x[n], 2) for n in range(3)]
        x2, = triangle(0, where, [set_x], cols(1), tri, last)
        o3 = swap(x2, 2)
        o1, = triangle(0, where, [set_o(1)], cols(0), tri, x2)
        y3 = swap(o1, 4)
        o2, = triangle(0, where, [set_o(2)], cols(1), tri, o1)
        x3 = swap(o2, 2)
        y1 = swap(o3, 4)
        xc, yc = pair(2, 0)
        x0, y0 = triangle(0, where, [xc, yc], [(b_o, 0, 48), (b_o2, 0, 48)], tri, o2, [(48, 1, 32, None, x0), (48, 1, 32, None, y0)])

        tiles = lambda *arrs: [(arr, 0) for arr in arrs]
        a_o1, b_o1 = project(1, [(48, tiles(o0, o1, o2, o3), rel, 0)], vectors, w_t, centre, 2, x0)
        b_o12 = swap(b_o1, 1)
        set_o = lambda z: [(a_o1, 0, 48, z, None)]
        a_x1, b_x1 = project(1, [(48, tiles(x0, x1, x2, x3), rel, 3)], vectors, w_t, centre, 2, a_o1)
        b_x12 = swap(b_x1, 1)
        b_y1, = project(1, [(48, tiles(y0, y1, y2, y3), rel, 6)], vectors, w_t, centre, 1, a_x1)
        b_y12 = swap(b_y1, 1)
        out, = triangle(1, where, [set_o(o0)], [(b_o1, 0, 48), (b_o12, 0, 48)], tri, b_y1, [(48, 4, 0, 0, None)])
        q2, = triangle(1, where, [[(a_x1, 0, 48, x2, None)]], [(b_y1, 0, 48), (b_y12, 0, 48)], tri, out)
        p3 = swap(q2, 2)
        out, = triangle(1, where, [set_o(o2)], [(b_y1, 0, 48), (b_y12, 0, 48)], tri, q2, [(48, 4, 0, 2, out)])
        out, = triangle(1, where, [set_o(o1)], [(b_x1, 0, 48), (b_x12, 0, 48)], tri, q2, [(48, 4, 0, 1, out)])
        out = lax.dynamic_update_slice(out, p3, (0, chip ^ 3, 0, 0))
        return out.reshape(48, 384, 128)

    return jax.shard_map(device_fn, mesh=mesh, in_specs=(row_spec, mask_spec, vec_spec, vec_spec, mat_spec, vec_spec, mat_spec, vec_spec, vec_spec, vec_spec, mat_spec, vec_spec), out_specs=row_spec, check_vma=False)
```

```python
import functools
import jax
import jax.numpy as jnp
from jax import lax
from jax.experimental import pallas as pl
from jax.experimental.pallas import tpu as pltpu
from jax.sharding import PartitionSpec as P

LN_EPS = 1e-5
ROWS = 16
CHUNK = 16
GROUP = 16
PITCH = 136
ROW_PITCH = 20
NT = (((1,), (1,)), ((), ()))


def norm_sublanes(x, scale, bias):
    mean = jnp.mean(x, axis=0, keepdims=True)
    xc = x - mean
    var = jnp.mean(xc * xc, axis=0, keepdims=True)
    return xc * lax.rsqrt(var + LN_EPS) * scale + bias


def project_kernel(layer, sides, team, sources, *refs):
    z_refs, refs = [refs[4 * n:4 * n + 4] for n in range(len(sources))], refs[4 * len(sources):]
    mask_refs, refs = refs[:len(sources)], refs[len(sources):]
    vectors, w_t, centre_in = refs[:3]
    outs = refs[4:4 + sides]
    proj, znt, stage, keep, mask, bias_ref, ln_s, ln_b, w_ref, centre, zbuf, obuf, load_sem, param_sem, out_sem = refs[4 + sides:]
    rows = sum(n for n, _, _ in sources)
    side0 = 512 - 256 * sides
    moves = [(centre_in, centre), (vectors.at[layer, 512:640], ln_s), (vectors.at[layer, 640:768], ln_b),
             (w_t.at[layer, side0:512], w_ref), (vectors.at[layer, side0:512], bias_ref)]
    at = 0
    for n, (count, _, mask_row) in enumerate(sources):
        moves.append((mask_refs[n].at[mask_row:mask_row + count], mask.at[at:at + count]))
        at += count
    params = [pltpu.make_async_copy(src, dst, param_sem.at[n]) for n, (src, dst) in enumerate(moves)]
    groups = rows // team

    def loads(n, first, g):
        copies = []
        for t in range(4):
            blk, row = sources[n][1][t]
            src = z_refs[n][t].at[pl.ds(pl.multiple_of(row + g * team, team), team), blk]
            dst = zbuf.at[pl.ds(pl.multiple_of(first + g * team, team), team), t]
            copies.append(pltpu.make_async_copy(src, dst, load_sem.at[first // team + g, t]))
        return copies

    for copy in params:
        copy.start()
    first = 0
    for n, (count, _, mask_row) in enumerate(sources):
        def start(g, carry, n=n, first=first):
            for copy in loads(n, first, g):
                copy.start()
            return carry

        lax.fori_loop(0, count // team, start, 0)
        first += count

    def arrive(g):
        for t in range(4):
            dst = zbuf.at[pl.ds(pl.multiple_of(g * team, team), team), t]
            pltpu.make_async_copy(z_refs[0][t].at[0:team, sources[0][1][t][0]], dst, load_sem.at[g, t]).wait()

    def normalise(g):
        z = zbuf[pl.ds(pl.multiple_of(g * team, team), team)].reshape(team * 384, 128)
        xc = lax.dot_general(centre[...], z, NT, preferred_element_type=jnp.float32)
        for lt in range(3 * team):
            ls = slice(lt * 128, lt * 128 + 128)
            x = xc[:, ls]
            var = jnp.mean(x * x, axis=0, keepdims=True)
            znt[:, ls] = (x * lax.rsqrt(var + LN_EPS) * ln_s[...] + ln_b[...]).astype(jnp.bfloat16)

    def stores(b, quarter):
        chans = pl.ds(pl.multiple_of(quarter * 32, 32), 32)
        at = pl.ds(pl.multiple_of(b * ROWS, ROWS), ROWS)
        return [pltpu.make_async_copy(obuf.at[b % 2, s, chans], outs[s].at[chans, at], out_sem.at[b % 2, s, quarter]) for s in range(sides)]

    arrive(0)
    for copy in params:
        copy.wait()
    keep[...] = mask[...].astype(jnp.float32).astype(jnp.bfloat16)
    normalise(0)

    def block(b, carry):
        def some(g, carry):
            after = b * (ROWS // team) + g + 1

            @pl.when(after < groups)
            def _():
                arrive(after)

            proj[...] = jnp.dot(w_ref[...], znt[...], preferred_element_type=jnp.float32)
            normalise(jnp.minimum(after, groups - 1))
            for h in range(team):
                i = g * team + h
                for lt in range(3):
                    ls = slice(h * 384 + lt * 128, h * 384 + lt * 128 + 128)
                    for s in range(sides):
                        value = proj[s * 256:s * 256 + 128, ls] + bias_ref[s * 256:s * 256 + 128]
                        gate = proj[s * 256 + 128:s * 256 + 256, ls] + bias_ref[s * 256 + 128:s * 256 + 256]
                        stage[s, lt, pl.ds(i, 128, stride=ROW_PITCH), :] = (jnp.tanh(gate) + 1.0) * value
            return carry

        lax.fori_loop(0, ROWS // team, some, 0)

        @pl.when(b >= 2)
        def _():
            for quarter in range(4):
                for copy in stores(b - 2, quarter):
                    copy.wait()

        m = keep[pl.ds(pl.multiple_of(b * ROWS, ROWS), ROWS)]

        def quarter_of(quarter, carry):
            def chan(c8, carry):
                c0 = quarter * 32 + c8 * 8
                for s in range(sides):
                    for lt in range(3):
                        view = stage.at[s, lt, pl.ds(pl.multiple_of(c0 * ROW_PITCH, 8), 8 * ROW_PITCH)]
                        for q in range(8):
                            obuf[b % 2, s, c0 + q, :, lt * 128:lt * 128 + 128] = view[q * ROW_PITCH:q * ROW_PITCH + ROWS].astype(jnp.bfloat16) * m[:, lt * 128:lt * 128 + 128]
                return carry

            lax.fori_loop(0, 4, chan, 0)
            for copy in stores(b, quarter):
                copy.start()
            return carry

        lax.fori_loop(0, 4, quarter_of, 0)
        return carry

    lax.fori_loop(0, rows // ROWS, block, 0)
    for b in range(max(rows // ROWS - 2, 0), rows // ROWS):
        for quarter in range(4):
            for copy in stores(b, quarter):
                copy.wait()


def project(layer, sources, vectors, w_t, centre, sides, dep, team=4):
    rows = sum(n for n, _, _, _ in sources)
    anywhere = pl.BlockSpec(memory_space=pl.ANY)
    in_specs = [anywhere] * (5 * len(sources) + 4)
    return pl.pallas_call(
        functools.partial(project_kernel, layer, sides, team, [(n, [tile[1:] for tile in tiles], at) for n, tiles, _, at in sources]),
        grid=(1,),
        out_shape=[jax.ShapeDtypeStruct((128, rows, 384), jnp.bfloat16)] * sides,
        in_specs=in_specs,
        out_specs=[anywhere] * sides,
        scratch_shapes=[pltpu.VMEM((256 * sides, team * 384), jnp.float32), pltpu.VMEM((128, team * 384), jnp.bfloat16), pltpu.VMEM((sides, 3, 128 * ROW_PITCH, 128), jnp.float32), pltpu.VMEM((rows, 384), jnp.bfloat16), pltpu.VMEM((rows, 384), jnp.int32),
                        pltpu.VMEM((256 * sides, 128), jnp.float32), pltpu.VMEM((128, 128), jnp.float32), pltpu.VMEM((128, 128), jnp.float32), pltpu.VMEM((256 * sides, 128), jnp.bfloat16), pltpu.VMEM((128, 128), jnp.bfloat16),
                        pltpu.VMEM((rows, 4, 96, 128), jnp.bfloat16), pltpu.VMEM((2, sides, 128, ROWS, 384), jnp.bfloat16),
                        pltpu.SemaphoreType.DMA((rows // team, 4)), pltpu.SemaphoreType.DMA((5 + len(sources),)), pltpu.SemaphoreType.DMA((2, sides, 4))],
        compiler_params=pltpu.CompilerParams(dimension_semantics=('arbitrary',), vmem_limit_bytes=62 * 2**20),
        cost_estimate=pl.CostEstimate(flops=rows * 384 * 128 * 512 * sides, bytes_accessed=rows * 384 * 256 * (1 + sides), transcendentals=0),
        name='project',
    )(*[tile[0] for _, tiles, _, _ in sources for tile in tiles], *[mask for _, _, mask, _ in sources], vectors, w_t, centre, dep)


def triangle_kernel(layer, jobs, n_a, n_b, n_z, n_out, n_held, where_ref, *refs):
    a_refs, refs = refs[:n_a], refs[n_a:]
    b_refs, refs = refs[:n_b], refs[n_b:]
    z_refs, refs = refs[:n_z], refs[n_z:]
    perm_in, centre_in, w_out_in, w_gate_in, vectors, rows_in = refs[:6]
    outs, refs = refs[6 + n_held:6 + n_held + n_out], refs[6 + n_held + n_out:]
    tri, abuf, bbuf, zbuf, obuf, perm_ref, centre, w_out, w_gate, ln_s, ln_b, rows_ref, load_sem, z_sem, param_sem, out_sem = refs
    b_out, b_gate, in_s, in_b = [rows_ref.at[n:n + 1] for n in range(4)]
    moves = [(perm_in, perm_ref), (centre_in, centre), (w_out_in.at[layer], w_out), (w_gate_in.at[layer], w_gate),
             (vectors.at[layer, 768:896], ln_s), (vectors.at[layer, 896:1024], ln_b), (rows_in.at[layer], rows_ref)]
    params = [pltpu.make_async_copy(src, dst, param_sem.at[n]) for n, (src, dst) in enumerate(moves)]
    column = lambda rel: 0 if rel is None else where_ref[0] ^ rel
    regions, z_at, zn, total = {}, [], [], 0
    for pieces, _, _ in jobs:
        z_at.append(total)
        zn.append(sum(len(p) for p, _, _ in jobs[:len(zn)]))
        total += sum(p[3] for p in pieces)

    a_at, loads_a, filled = [], [], 0
    for pieces, _, _ in jobs:
        key = tuple(p[1:4] for p in pieces)
        loads_a.append(key not in regions)
        if key not in regions:
            regions[key] = filled
            filled += sum(p[3] for p in pieces)
        a_at.append(regions[key])

    def loads(j, q):
        pieces, b_pieces, _ = jobs[j]
        chans = pl.ds(pl.multiple_of(q * CHUNK, CHUNK), CHUNK)
        copies, r0 = [], a_at[j]
        for n, (_, a, blk, count, _, _) in enumerate(pieces if loads_a[j] else ()):
            copies.append(pltpu.make_async_copy(a_refs[a].at[chans, blk * count:blk * count + count], abuf.at[chans, r0:r0 + count], load_sem.at[j, q, n]))
            r0 += count
        r0 = 0
        for n, (b, blk, count) in enumerate(b_pieces):
            copies.append(pltpu.make_async_copy(b_refs[b].at[chans, blk * count:blk * count + count], bbuf.at[j, chans, r0:r0 + count], load_sem.at[j, q, len(pieces) + n]))
            r0 += count
        return copies

    def z_loads(j):
        copies, r0 = [], z_at[j]
        for n, (_, _, _, count, rel, z0) in enumerate(jobs[j][0]):
            copies.append(pltpu.make_async_copy(z_refs[zn[j] + n].at[z0:z0 + count, column(rel)], zbuf.at[r0:r0 + count], z_sem.at[zn[j] + n]))
            r0 += count
        return copies

    for j in range(len(jobs)):
        def start_loads(q, carry, j=j):
            for copy in loads(j, q):
                copy.start()
            return carry

        lax.fori_loop(0, 128 // CHUNK, start_loads, 0)
        for copy in z_loads(j) + (params if j == 0 else []):
            copy.start()
    tri[:, 96:128] = jnp.zeros((tri.shape[0], 32), jnp.float32)

    def some_rows(i0, at):
        flipped = []
        for q in range(GROUP):
            o = tri[pl.ds(pl.multiple_of((i0 + q) * PITCH, 8), 128), :]
            on = norm_sublanes(o, ln_s[...], ln_b[...]).astype(jnp.bfloat16)
            flipped.append(lax.dot_general(perm_ref[...], on, NT, preferred_element_type=jnp.float32).astype(jnp.bfloat16))
        on = jnp.concatenate(flipped, axis=0)
        u = jnp.dot(on, w_out[...], preferred_element_type=jnp.float32) + b_out[...]
        u = u.astype(jnp.bfloat16).astype(jnp.float32)
        zb = zbuf[pl.ds(at, GROUP)].reshape(GROUP * 96, 128)
        xc = jnp.dot(zb, centre[...], preferred_element_type=jnp.float32)
        z = zb.astype(jnp.float32)
        var = jnp.mean(xc * xc, axis=-1, keepdims=True)
        zn = (xc * lax.rsqrt(var + LN_EPS) * in_s[...] + in_b[...]).astype(jnp.bfloat16)
        g = jnp.dot(zn, w_gate[...], preferred_element_type=jnp.float32) + b_gate[...]
        g = 0.5 * jnp.tanh(g) + 0.5
        obuf[pl.ds(at, GROUP)] = (z + g * u).astype(jnp.bfloat16).reshape(GROUP, 96, 128)

    written = []
    for j, (pieces, b_pieces, outputs) in enumerate(jobs):
        rows = sum(p[3] for p in pieces)

        def some_channels(q, carry, j=j, rows=rows):
            for copy in loads(j, q):
                copy.wait()
            for cc in range(CHUNK):
                c = q * CHUNK + cc
                o = lax.dot_general(abuf[c, a_at[j]:a_at[j] + rows], bbuf[j, c], NT, preferred_element_type=jnp.float32)
                tri[pl.ds(c, rows, stride=PITCH), 0:96] = o
            return carry

        lax.fori_loop(0, 128 // CHUNK, some_channels, 0)
        for copy in z_loads(j) + (params if j == 0 else []):
            copy.wait()

        spans, r0 = [], 0
        for s, _, _, count, _, _ in pieces:
            if spans and spans[-1][0] == s:
                spans[-1][2] += count
            else:
                spans.append([s, r0, count])
            r0 += count

        def store(s, r0, i, j=j, outputs=outputs):
            arr, first, rel = outputs[s]
            row, to = pl.multiple_of(z_at[j] + r0 + i * GROUP, GROUP), pl.multiple_of(first + i * GROUP, GROUP)
            return pltpu.make_async_copy(obuf.at[pl.ds(row, GROUP)], outs[arr].at[pl.ds(to, GROUP), column(rel)], out_sem.at[(z_at[j] + r0) // GROUP + i])

        for s, r0, count in spans:
            def body(i, carry, s=s, r0=r0, store=store, j=j):
                i0 = pl.multiple_of(r0 + i * GROUP, GROUP)
                some_rows(i0, z_at[j] + i0)
                store(s, r0, i).start()
                return carry

            lax.fori_loop(0, count // GROUP, body, 0)
            written += [(store, s, r0, i) for i in range(count // GROUP)]
    for store, s, r0, i in written:
        store(s, r0, i).wait()


def triangles(layer, where, jobs, arrays, params, dep):
    def place(arr, pool):
        for n, other in enumerate(pool):
            if other is arr:
                return n
        pool.append(arr)
        return len(pool) - 1

    a_pool, b_pool, z_pool, static, most_b, most_a = [], [], [], [], 0, 0
    for pieces, b_pieces, outputs in jobs:
        z_pool += [p[4] for p in pieces]
        static.append(([(p[0], place(p[1], a_pool), p[2], p[3], p[5], p[6]) for p in pieces],
                       [(place(b, b_pool), blk, n) for b, blk, n in b_pieces], outputs))
        most_a, most_b = max(most_a, len(pieces)), max(most_b, len(b_pieces))
    total = sum(p[3] for pieces, _, _ in static for p in pieces)
    rows = max(sum(p[3] for p in pieces) for pieces, _, _ in static)
    keys = {tuple(p[1:4] for p in pieces) for pieces, _, _ in static}
    held_rows = sum(n for key in keys for _, _, n in key)
    deps = dep if isinstance(dep, tuple) else (dep,)
    held = [prev for _, _, prev in arrays if prev is not None]
    first = 1 + len(a_pool) + len(b_pool) + len(z_pool) + len(params) + len(deps)
    aliases, seen = {}, 0
    for s, (_, _, prev) in enumerate(arrays):
        if prev is not None:
            aliases[first + seen] = s
            seen += 1
    anywhere = pl.BlockSpec(memory_space=pl.ANY)
    in_specs = [anywhere] * (len(a_pool) + len(b_pool) + len(z_pool) + len(params) + len(deps) + len(held))
    return pl.pallas_call(
        functools.partial(triangle_kernel, layer, static, len(a_pool), len(b_pool), len(z_pool), len(arrays), len(deps) + len(held)),
        out_shape=[jax.ShapeDtypeStruct((n, width, 96, 128), jnp.bfloat16) for n, width, _ in arrays],
        input_output_aliases=aliases,
        grid_spec=pltpu.PrefetchScalarGridSpec(
            num_scalar_prefetch=1, grid=(1,), in_specs=in_specs, out_specs=[anywhere] * len(arrays),
            scratch_shapes=[pltpu.VMEM((rows * PITCH, 128), jnp.float32), pltpu.VMEM((128, held_rows, 384), jnp.bfloat16), pltpu.VMEM((len(jobs), 128, 96, 384), jnp.bfloat16),
                            pltpu.VMEM((total, 96, 128), jnp.bfloat16), pltpu.VMEM((total, 96, 128), jnp.bfloat16),
                            pltpu.VMEM((96, 128), jnp.bfloat16), pltpu.VMEM((128, 128), jnp.bfloat16), pltpu.VMEM((128, 128), jnp.bfloat16), pltpu.VMEM((128, 128), jnp.bfloat16),
                            pltpu.VMEM((128, 128), jnp.float32), pltpu.VMEM((128, 128), jnp.float32), pltpu.VMEM((4, 128), jnp.float32),
                            pltpu.SemaphoreType.DMA((len(jobs), 128 // CHUNK, most_a + most_b)), pltpu.SemaphoreType.DMA((len(z_pool),)), pltpu.SemaphoreType.DMA((7,)), pltpu.SemaphoreType.DMA((total // GROUP,))]),
        compiler_params=pltpu.CompilerParams(dimension_semantics=('arbitrary',), vmem_limit_bytes=62 * 2**20),
        cost_estimate=pl.CostEstimate(flops=total * 96 * 128 * 1800, bytes_accessed=(total + 96) * 384 * 256, transcendentals=0),
        name='triangle',
    )(where, *a_pool, *b_pool, *z_pool, *params, *deps, *held)


def triangle(layer, where, sets, b_pieces, params, dep, into=None):
    into = into or [(sum(p[2] for p in pieces), 1, 0, None, None) for pieces in sets]
    job = ([(s,) + p for s, pieces in enumerate(sets) for p in pieces], b_pieces, [(s, at, rel) for s, (_, _, at, rel, _) in enumerate(into)])
    return triangles(layer, where, [job], [(n, width, prev) for n, width, _, _, prev in into], params, dep)


def solution(mesh):
    row_spec = P(('batch', 'dap'), None, None)
    mask_spec = P(('batch', 'dap'), None)
    vec_spec = P(None, None)
    mat_spec = P(None, None, None)

    def swap(x, bit):
        return lax.ppermute(x, 'dap', [(i, i ^ bit) for i in range(8)])

    def device_fn(z_rows, mask_rows, ln_in_scale, ln_in_bias, w_in, b_in, w_gate, b_gate, ln_out_scale, ln_out_bias, w_out, b_out):
        f32, bf16 = jnp.float32, jnp.bfloat16
        index = lax.axis_index('dap')
        chip, core = index // 2, index % 2
        z_own = z_rows.reshape(48, 4, 96, 128)
        z_x, z_y = [], []
        for n in range(3):
            part = (z_own if n == 0 else lax.optimization_barrier(z_own))[16 * n:16 * n + 16]
            z_x.append(swap(part, 2))
            z_y.append(swap(part, 4))
        mask_bf = mask_rows
        mask_x, mask_y = swap(mask_bf, 2), swap(mask_bf, 4)
        masks = [mask_bf, mask_x, mask_y]
        cut = lambda m, n: [m[:, i * n:i * n + n] for i in range(384 // n)]
        rel = jnp.concatenate(masks, axis=0)
        h = cut(rel, 192)
        rel = jnp.where(chip >= 2, jnp.concatenate([h[1], h[0]], axis=1), rel)
        q = cut(rel, 96)
        rel = jnp.where(chip % 2 == 1, jnp.concatenate([q[1], q[0], q[3], q[2]], axis=1), rel)
        j = jnp.arange(96)
        source = jnp.where(core == 0, j, (j + 48) % 96)
        perm = (source[:, None] == jnp.arange(128)[None, :]).astype(bf16)
        eye = jnp.arange(128)[:, None] == jnp.arange(128)[None, :]
        centre = (eye.astype(f32) - 1.0 / 128).astype(bf16)
        zero = jnp.zeros((1,), jnp.int32)
        where = jnp.reshape(chip, (1,)).astype(jnp.int32)
        vectors = jnp.concatenate([b_in.astype(f32) * 0.5] + [v.astype(f32) for v in (ln_in_scale, ln_in_bias, ln_out_scale, ln_out_bias)], axis=1)
        vectors = jnp.broadcast_to(vectors[:, :, None], (2, 1024, 128))
        rows4 = jnp.stack([b_out.astype(f32), b_gate.astype(f32) * 0.5, ln_in_scale.astype(f32), ln_in_bias.astype(f32)], axis=1)
        w_t = jnp.swapaxes(w_in * bf16(0.5), 1, 2)
        tri = (perm, centre, w_out, w_gate * bf16(0.5), vectors, rows4)
        spread = lambda arr: [(arr, i, 0) for i in range(4)]
        a_o, b_o = project(0, [(48, spread(z_own), mask_bf, 0)], vectors, w_t, centre, 2, perm)
        b_o2 = swap(b_o, 1)
        own = [(b_o, 0, 48), (b_o2, 0, 48)]
        o0, = triangle(0, where, [[(a_o, 0, 48, z_own, 0, 0)]], own, tri, a_o)
        x1, y2 = swap(o0, 2), swap(o0, 4)
        parts, last = [], o0
        for n in range(3):
            if n == 2:
                pair = lambda m, rel: ([(parts[m][0], 0, 16, z_x[m], rel, 0)], [(parts[m][0], 1, 16, z_y[m], rel, 0)])
                (xa, ya), (xb, yb) = pair(0, 0), pair(1, 0)
                x0, y0 = triangle(0, where, [xa + xb, ya + yb], own, tri, (last, rel), [(48, 1, 0, None, None)] * 2)
                last = x0
            a_n, b_n = project(0, [(16, spread(z_x[n]), mask_x, 16 * n), (16, spread(z_y[n]), mask_y, 16 * n)], vectors, w_t, centre, 2, last)
            parts.append((a_n, b_n, swap(b_n, 1)))
            last = a_n
        cols = lambda k: [(p[1], k, 16) for p in parts] + [(p[2], k, 16) for p in parts]
        piece_x = [(parts[n][0], 0, 16, z_x[n], 2, 0) for n in range(3)]
        x2, = triangle(0, where, [piece_x], cols(1), tri, last)
        o3 = swap(x2, 2)
        o1, = triangle(0, where, [[(a_o, 0, 48, z_own, 1, 0)]], cols(0), tri, x2)
        y3 = swap(o1, 4)
        o2, = triangle(0, where, [[(a_o, 0, 48, z_own, 2, 0)]], cols(1), tri, o1)
        x3 = swap(o2, 2)
        y1 = swap(o3, 4)
        xc, yc = pair(2, 0)
        x0, y0 = triangle(0, where, [xc, yc], own, tri, o2, [(48, 1, 32, None, x0), (48, 1, 32, None, y0)])

        tiles = lambda row, *arrs: [(arr, 0, row) for arr in arrs]
        a_o, b_o = project(1, [(48, tiles(0, o0, o1, o2, o3), rel, 0)], vectors, w_t, centre, 2, x0, 8)
        b_o2 = swap(b_o, 1)
        a_x, b_x = project(1, [(48, tiles(0, x0, x1, x2, x3), rel, 48)], vectors, w_t, centre, 2, a_o, 8)
        b_x2 = swap(b_x, 1)
        b_ya, = project(1, [(32, tiles(0, y0, y1, y2, y3), rel, 96)], vectors, w_t, centre, 1, a_x)
        b_ya2 = swap(b_ya, 1)
        b_yb, = project(1, [(16, tiles(32, y0, y1, y2, y3), rel, 128)], vectors, w_t, centre, 1, b_ya)
        b_yb2 = swap(b_yb, 1)
        own, col_x = [(b_o, 0, 48), (b_o2, 0, 48)], [(b_x, 0, 48), (b_x2, 0, 48)]
        col_y = [(b_ya, 0, 32), (b_yb, 0, 16), (b_ya2, 0, 32), (b_yb2, 0, 16)]
        q2, = triangle(1, where, [[(a_x, 0, 48, x2, None, 0)]], col_y, tri, b_yb)
        p3 = swap(q2, 2)
        out, = triangles(1, where, [
            ([(0, a_o, 0, 48, o0, None, 0)], own, [(0, 0, 0)]),
            ([(0, a_o, 0, 48, o1, None, 0)], col_x, [(0, 0, 1)]),
            ([(0, a_o, 0, 48, o2, None, 0)], col_y, [(0, 0, 2)]),
        ], [(48, 4, None)], tri, q2)
        out = lax.dynamic_update_slice(out, p3, (0, chip ^ 3, 0, 0))
        return out.reshape(48, 384, 128)

    return jax.shard_map(device_fn, mesh=mesh, in_specs=(row_spec, mask_spec, vec_spec, vec_spec, mat_spec, vec_spec, mat_spec, vec_spec, vec_spec, vec_spec, mat_spec, vec_spec), out_specs=row_spec, check_vma=False)
```

```python
import functools
import jax
import jax.numpy as jnp
from jax import lax
from jax.experimental import pallas as pl
from jax.experimental.pallas import tpu as pltpu
from jax.sharding import PartitionSpec as P

LN_EPS = 1e-5
ROWS = 16
CHUNK = 16
GROUP = 16
PITCH = 136
CH = 128
OWN = 48
VMEM_BYTES = 67043328
ROW_PITCH = 20
NT = (((1,), (1,)), ((), ()))


def norm_sublanes(x, scale, bias):
    mean = jnp.mean(x, axis=0, keepdims=True)
    xc = x - mean
    var = jnp.mean(xc * xc, axis=0, keepdims=True)
    return xc * lax.rsqrt(var + LN_EPS) * scale + bias


def project_kernel(layer, sides, team, sources, *refs):
    z_refs, refs = [refs[4 * n:4 * n + 4] for n in range(len(sources))], refs[4 * len(sources):]
    mask_refs, refs = refs[:len(sources)], refs[len(sources):]
    vectors, w_t, centre_in = refs[:3]
    outs = refs[4:4 + sides]
    proj, znt, stage, keep, mask, bias_ref, ln_s, ln_b, w_ref, centre, zbuf, obuf, load_sem, param_sem, out_sem = refs[4 + sides:]
    rows = sum(n for n, _, _ in sources)
    side0 = 512 - 256 * sides
    moves = [(centre_in, centre), (vectors.at[layer, 512:640], ln_s), (vectors.at[layer, 640:768], ln_b),
             (w_t.at[layer, side0:512], w_ref), (vectors.at[layer, side0:512], bias_ref)]
    at = 0
    for n, (count, _, mask_row) in enumerate(sources):
        moves.append((mask_refs[n].at[mask_row:mask_row + count], mask.at[at:at + count]))
        at += count
    params = [pltpu.make_async_copy(src, dst, param_sem.at[n]) for n, (src, dst) in enumerate(moves)]
    groups = rows // team

    def loads(n, first, g):
        copies = []
        for t in range(4):
            blk, row = sources[n][1][t]
            src = z_refs[n][t].at[pl.ds(pl.multiple_of(row + g * team, team), team), blk]
            dst = zbuf.at[pl.ds(pl.multiple_of(first + g * team, team), team), t]
            copies.append(pltpu.make_async_copy(src, dst, load_sem.at[first // team + g, t]))
        return copies

    for copy in params:
        copy.start()
    first = 0
    for n, (count, _, mask_row) in enumerate(sources):
        def start(g, carry, n=n, first=first):
            for copy in loads(n, first, g):
                copy.start()
            return carry

        lax.fori_loop(0, count // team, start, 0)
        first += count

    def arrive(g):
        for t in range(4):
            dst = zbuf.at[pl.ds(pl.multiple_of(g * team, team), team), t]
            pltpu.make_async_copy(z_refs[0][t].at[0:team, sources[0][1][t][0]], dst, load_sem.at[g, t]).wait()

    def normalise(g):
        z = zbuf[pl.ds(pl.multiple_of(g * team, team), team)].reshape(team * 384, CH)
        xc = lax.dot_general(centre[...], z, NT, preferred_element_type=jnp.float32)
        for lt in range(3 * team):
            ls = slice(lt * CH, lt * CH + CH)
            x = xc[:, ls]
            var = jnp.mean(x * x, axis=0, keepdims=True)
            znt[:, ls] = (x * lax.rsqrt(var + LN_EPS) * ln_s[...] + ln_b[...]).astype(jnp.bfloat16)

    def stores(b, quarter):
        chans = pl.ds(pl.multiple_of(quarter * 32, 32), 32)
        at = pl.ds(pl.multiple_of(b * ROWS, ROWS), ROWS)
        return [pltpu.make_async_copy(obuf.at[b % 2, s, chans], outs[s].at[chans, at], out_sem.at[b % 2, s, quarter]) for s in range(sides)]

    arrive(0)
    for copy in params:
        copy.wait()
    keep[...] = mask[...].astype(jnp.float32).astype(jnp.bfloat16)
    normalise(0)

    def block(b, carry):
        def some(g, carry):
            after = b * (ROWS // team) + g + 1

            @pl.when(after < groups)
            def _():
                arrive(after)

            proj[...] = jnp.dot(w_ref[...], znt[...], preferred_element_type=jnp.float32)
            normalise(jnp.minimum(after, groups - 1))
            for h in range(team):
                i = g * team + h
                for lt in range(3):
                    ls = slice(h * 384 + lt * CH, h * 384 + lt * CH + CH)
                    for s in range(sides):
                        value = proj[s * 256:s * 256 + CH, ls] + bias_ref[s * 256:s * 256 + CH]
                        gate = proj[s * 256 + CH:s * 256 + 256, ls] + bias_ref[s * 256 + CH:s * 256 + 256]
                        stage[s, lt, pl.ds(i, CH, stride=ROW_PITCH), :] = (jnp.tanh(gate) + 1.0) * value
            return carry

        lax.fori_loop(0, ROWS // team, some, 0)

        @pl.when(b >= 2)
        def _():
            for quarter in range(4):
                for copy in stores(b - 2, quarter):
                    copy.wait()

        m = keep[pl.ds(pl.multiple_of(b * ROWS, ROWS), ROWS)]

        def quarter_of(quarter, carry):
            def chan(c8, carry):
                c0 = quarter * 32 + c8 * 8
                for s in range(sides):
                    for lt in range(3):
                        view = stage.at[s, lt, pl.ds(pl.multiple_of(c0 * ROW_PITCH, 8), 8 * ROW_PITCH)]
                        for q in range(8):
                            obuf[b % 2, s, c0 + q, :, lt * CH:lt * CH + CH] = view[q * ROW_PITCH:q * ROW_PITCH + ROWS].astype(jnp.bfloat16) * m[:, lt * CH:lt * CH + CH]
                return carry

            lax.fori_loop(0, 4, chan, 0)
            for copy in stores(b, quarter):
                copy.start()
            return carry

        lax.fori_loop(0, 4, quarter_of, 0)
        return carry

    lax.fori_loop(0, rows // ROWS, block, 0)
    for b in range(max(rows // ROWS - 2, 0), rows // ROWS):
        for quarter in range(4):
            for copy in stores(b, quarter):
                copy.wait()


def project(layer, sources, vectors, w_t, centre, sides, dep, team=4):
    rows = sum(n for n, _, _, _ in sources)
    anywhere = pl.BlockSpec(memory_space=pl.ANY)
    in_specs = [anywhere] * (5 * len(sources) + 4)
    return pl.pallas_call(
        functools.partial(project_kernel, layer, sides, team, [(n, [tile[1:] for tile in tiles], at) for n, tiles, _, at in sources]),
        grid=(1,),
        out_shape=[jax.ShapeDtypeStruct((CH, rows, 384), jnp.bfloat16)] * sides,
        in_specs=in_specs,
        out_specs=[anywhere] * sides,
        scratch_shapes=[pltpu.VMEM((256 * sides, team * 384), jnp.float32), pltpu.VMEM((CH, team * 384), jnp.bfloat16), pltpu.VMEM((sides, 3, CH * ROW_PITCH, CH), jnp.float32), pltpu.VMEM((rows, 384), jnp.bfloat16), pltpu.VMEM((rows, 384), jnp.int32),
                        pltpu.VMEM((256 * sides, CH), jnp.float32), pltpu.VMEM((CH, CH), jnp.float32), pltpu.VMEM((CH, CH), jnp.float32), pltpu.VMEM((256 * sides, CH), jnp.bfloat16), pltpu.VMEM((CH, CH), jnp.bfloat16),
                        pltpu.VMEM((rows, 4, 96, CH), jnp.bfloat16), pltpu.VMEM((2, sides, CH, ROWS, 384), jnp.bfloat16),
                        pltpu.SemaphoreType.DMA((rows // team, 4)), pltpu.SemaphoreType.DMA((5 + len(sources),)), pltpu.SemaphoreType.DMA((2, sides, 4))],
        compiler_params=pltpu.CompilerParams(dimension_semantics=('arbitrary',), vmem_limit_bytes=VMEM_BYTES),
        cost_estimate=pl.CostEstimate(flops=rows * 384 * CH * 512 * sides, bytes_accessed=rows * 384 * 256 * (1 + sides), transcendentals=0),
        name='project',
    )(*[tile[0] for _, tiles, _, _ in sources for tile in tiles], *[mask for _, _, mask, _ in sources], vectors, w_t, centre, dep)


def triangle_kernel(layer, jobs, n_a, n_b, n_z, n_out, n_held, where_ref, *refs):
    a_refs, refs = refs[:n_a], refs[n_a:]
    b_refs, refs = refs[:n_b], refs[n_b:]
    z_refs, refs = refs[:n_z], refs[n_z:]
    perm_in, centre_in, w_out_in, w_gate_in, vectors, rows_in = refs[:6]
    outs, refs = refs[6 + n_held:6 + n_held + n_out], refs[6 + n_held + n_out:]
    tri, abuf, bbuf, zbuf, obuf, perm_ref, centre, w_out, w_gate, ln_s, ln_b, rows_ref, load_sem, z_sem, param_sem, out_sem = refs
    b_out, b_gate, in_s, in_b = [rows_ref.at[n:n + 1] for n in range(4)]
    moves = [(perm_in, perm_ref), (centre_in, centre), (w_out_in.at[layer], w_out), (w_gate_in.at[layer], w_gate),
             (vectors.at[layer, 768:896], ln_s), (vectors.at[layer, 896:1024], ln_b), (rows_in.at[layer], rows_ref)]
    params = [pltpu.make_async_copy(src, dst, param_sem.at[n]) for n, (src, dst) in enumerate(moves)]
    column = lambda rel: 0 if rel is None else where_ref[0] ^ rel
    regions, z_at, zn, total = {}, [], [], 0
    for pieces, _, _ in jobs:
        z_at.append(total)
        zn.append(sum(len(p) for p, _, _ in jobs[:len(zn)]))
        total += sum(p[3] for p in pieces)

    a_at, loads_a, filled = [], [], 0
    for pieces, _, _ in jobs:
        key = tuple(p[1:4] for p in pieces)
        loads_a.append(key not in regions)
        if key not in regions:
            regions[key] = filled
            filled += sum(p[3] for p in pieces)
        a_at.append(regions[key])

    def loads(j, q):
        pieces, b_pieces, _ = jobs[j]
        chans = pl.ds(pl.multiple_of(q * CHUNK, CHUNK), CHUNK)
        copies, r0 = [], a_at[j]
        for n, (_, a, blk, count, _, _) in enumerate(pieces if loads_a[j] else ()):
            copies.append(pltpu.make_async_copy(a_refs[a].at[chans, blk * count:blk * count + count], abuf.at[chans, r0:r0 + count], load_sem.at[j, q, n]))
            r0 += count
        r0 = 0
        for n, (b, blk, count) in enumerate(b_pieces):
            copies.append(pltpu.make_async_copy(b_refs[b].at[chans, blk * count:blk * count + count], bbuf.at[j, chans, r0:r0 + count], load_sem.at[j, q, len(pieces) + n]))
            r0 += count
        return copies

    def z_loads(j):
        copies, r0 = [], z_at[j]
        for n, (_, _, _, count, rel, z0) in enumerate(jobs[j][0]):
            copies.append(pltpu.make_async_copy(z_refs[zn[j] + n].at[z0:z0 + count, column(rel)], zbuf.at[r0:r0 + count], z_sem.at[zn[j] + n]))
            r0 += count
        return copies

    for j in range(len(jobs)):
        def start_loads(q, carry, j=j):
            for copy in loads(j, q):
                copy.start()
            return carry

        lax.fori_loop(0, CH // CHUNK, start_loads, 0)
        for copy in z_loads(j) + (params if j == 0 else []):
            copy.start()
    tri[:, 96:CH] = jnp.zeros((tri.shape[0], 32), jnp.float32)

    def some_rows(i0, at):
        flipped = []
        for q in range(GROUP):
            o = tri[pl.ds(pl.multiple_of((i0 + q) * PITCH, 8), CH), :]
            on = norm_sublanes(o, ln_s[...], ln_b[...]).astype(jnp.bfloat16)
            flipped.append(lax.dot_general(perm_ref[...], on, NT, preferred_element_type=jnp.float32).astype(jnp.bfloat16))
        on = jnp.concatenate(flipped, axis=0)
        u = jnp.dot(on, w_out[...], preferred_element_type=jnp.float32) + b_out[...]
        u = u.astype(jnp.bfloat16).astype(jnp.float32)
        zb = zbuf[pl.ds(at, GROUP)].reshape(GROUP * 96, CH)
        xc = jnp.dot(zb, centre[...], preferred_element_type=jnp.float32)
        z = zb.astype(jnp.float32)
        var = jnp.mean(xc * xc, axis=-1, keepdims=True)
        zn = (xc * lax.rsqrt(var + LN_EPS) * in_s[...] + in_b[...]).astype(jnp.bfloat16)
        g = jnp.dot(zn, w_gate[...], preferred_element_type=jnp.float32) + b_gate[...]
        g = 0.5 * jnp.tanh(g) + 0.5
        obuf[pl.ds(at, GROUP)] = (z + g * u).astype(jnp.bfloat16).reshape(GROUP, 96, CH)

    written = []
    for j, (pieces, b_pieces, outputs) in enumerate(jobs):
        rows = sum(p[3] for p in pieces)

        def some_channels(q, carry, j=j, rows=rows):
            for copy in loads(j, q):
                copy.wait()
            for cc in range(CHUNK):
                c = q * CHUNK + cc
                o = lax.dot_general(abuf[c, a_at[j]:a_at[j] + rows], bbuf[j, c], NT, preferred_element_type=jnp.float32)
                tri[pl.ds(c, rows, stride=PITCH), 0:96] = o
            return carry

        lax.fori_loop(0, CH // CHUNK, some_channels, 0)
        for copy in z_loads(j) + (params if j == 0 else []):
            copy.wait()

        spans, r0 = [], 0
        for s, _, _, count, _, _ in pieces:
            if spans and spans[-1][0] == s:
                spans[-1][2] += count
            else:
                spans.append([s, r0, count])
            r0 += count

        def store(s, r0, i, j=j, outputs=outputs):
            arr, first, rel = outputs[s]
            row, to = pl.multiple_of(z_at[j] + r0 + i * GROUP, GROUP), pl.multiple_of(first + i * GROUP, GROUP)
            return pltpu.make_async_copy(obuf.at[pl.ds(row, GROUP)], outs[arr].at[pl.ds(to, GROUP), column(rel)], out_sem.at[(z_at[j] + r0) // GROUP + i])

        for s, r0, count in spans:
            def body(i, carry, s=s, r0=r0, store=store, j=j):
                i0 = pl.multiple_of(r0 + i * GROUP, GROUP)
                some_rows(i0, z_at[j] + i0)
                store(s, r0, i).start()
                return carry

            lax.fori_loop(0, count // GROUP, body, 0)
            written += [(store, s, r0, i) for i in range(count // GROUP)]
    for store, s, r0, i in written:
        store(s, r0, i).wait()


def triangles(layer, where, jobs, arrays, params, dep):
    def place(arr, pool):
        for n, other in enumerate(pool):
            if other is arr:
                return n
        pool.append(arr)
        return len(pool) - 1

    a_pool, b_pool, z_pool, static, most_b, most_a = [], [], [], [], 0, 0
    for pieces, b_pieces, outputs in jobs:
        z_pool += [p[4] for p in pieces]
        static.append(([(p[0], place(p[1], a_pool), p[2], p[3], p[5], p[6]) for p in pieces],
                       [(place(b, b_pool), blk, n) for b, blk, n in b_pieces], outputs))
        most_a, most_b = max(most_a, len(pieces)), max(most_b, len(b_pieces))
    total = sum(p[3] for pieces, _, _ in static for p in pieces)
    rows = max(sum(p[3] for p in pieces) for pieces, _, _ in static)
    keys = {tuple(p[1:4] for p in pieces) for pieces, _, _ in static}
    held_rows = sum(n for key in keys for _, _, n in key)
    deps = dep if isinstance(dep, tuple) else (dep,)
    held = [prev for _, _, prev in arrays if prev is not None]
    first = 1 + len(a_pool) + len(b_pool) + len(z_pool) + len(params) + len(deps)
    aliases, seen = {}, 0
    for s, (_, _, prev) in enumerate(arrays):
        if prev is not None:
            aliases[first + seen] = s
            seen += 1
    anywhere = pl.BlockSpec(memory_space=pl.ANY)
    in_specs = [anywhere] * (len(a_pool) + len(b_pool) + len(z_pool) + len(params) + len(deps) + len(held))
    return pl.pallas_call(
        functools.partial(triangle_kernel, layer, static, len(a_pool), len(b_pool), len(z_pool), len(arrays), len(deps) + len(held)),
        out_shape=[jax.ShapeDtypeStruct((n, width, 96, CH), jnp.bfloat16) for n, width, _ in arrays],
        input_output_aliases=aliases,
        grid_spec=pltpu.PrefetchScalarGridSpec(
            num_scalar_prefetch=1, grid=(1,), in_specs=in_specs, out_specs=[anywhere] * len(arrays),
            scratch_shapes=[pltpu.VMEM((rows * PITCH, CH), jnp.float32), pltpu.VMEM((CH, held_rows, 384), jnp.bfloat16), pltpu.VMEM((len(jobs), CH, 96, 384), jnp.bfloat16),
                            pltpu.VMEM((total, 96, CH), jnp.bfloat16), pltpu.VMEM((total, 96, CH), jnp.bfloat16),
                            pltpu.VMEM((96, CH), jnp.bfloat16), pltpu.VMEM((CH, CH), jnp.bfloat16), pltpu.VMEM((CH, CH), jnp.bfloat16), pltpu.VMEM((CH, CH), jnp.bfloat16),
                            pltpu.VMEM((CH, CH), jnp.float32), pltpu.VMEM((CH, CH), jnp.float32), pltpu.VMEM((4, CH), jnp.float32),
                            pltpu.SemaphoreType.DMA((len(jobs), CH // CHUNK, most_a + most_b)), pltpu.SemaphoreType.DMA((len(z_pool),)), pltpu.SemaphoreType.DMA((7,)), pltpu.SemaphoreType.DMA((total // GROUP,))]),
        compiler_params=pltpu.CompilerParams(dimension_semantics=('arbitrary',), vmem_limit_bytes=VMEM_BYTES),
        cost_estimate=pl.CostEstimate(flops=total * 96 * CH * 1800, bytes_accessed=(total + 96) * 384 * 256, transcendentals=0),
        name='triangle',
    )(where, *a_pool, *b_pool, *z_pool, *params, *deps, *held)


def triangle(layer, where, sets, b_pieces, params, dep, into=None):
    into = into or [(sum(p[2] for p in pieces), 1, 0, None, None) for pieces in sets]
    job = ([(s,) + p for s, pieces in enumerate(sets) for p in pieces], b_pieces, [(s, at, rel) for s, (_, _, at, rel, _) in enumerate(into)])
    return triangles(layer, where, [job], [(n, width, prev) for n, width, _, _, prev in into], params, dep)


def solution(mesh):
    row_spec = P(('batch', 'dap'), None, None)
    mask_spec = P(('batch', 'dap'), None)
    vec_spec = P(None, None)
    mat_spec = P(None, None, None)

    def swap(x, bit):
        return lax.ppermute(x, 'dap', [(i, i ^ bit) for i in range(8)])

    def device_fn(z_rows, mask_rows, ln_in_scale, ln_in_bias, w_in, b_in, w_gate, b_gate, ln_out_scale, ln_out_bias, w_out, b_out):
        f32, bf16 = jnp.float32, jnp.bfloat16
        index = lax.axis_index('dap')
        chip, core = index // 2, index % 2
        z_own = z_rows.reshape(OWN, 4, 96, CH)
        z_x, z_y = [], []
        for n in range(3):
            part = (z_own if n == 0 else lax.optimization_barrier(z_own))[16 * n:16 * n + 16]
            z_x.append(swap(part, 2))
            z_y.append(swap(part, 4))
        mask_bf = mask_rows
        mask_x, mask_y = swap(mask_bf, 2), swap(mask_bf, 4)
        masks = [mask_bf, mask_x, mask_y]
        cut = lambda m, n: [m[:, i * n:i * n + n] for i in range(384 // n)]
        rel = jnp.concatenate(masks, axis=0)
        h = cut(rel, 192)
        rel = jnp.where(chip >= 2, jnp.concatenate([h[1], h[0]], axis=1), rel)
        q = cut(rel, 96)
        rel = jnp.where(chip % 2 == 1, jnp.concatenate([q[1], q[0], q[3], q[2]], axis=1), rel)
        j = jnp.arange(96)
        source = jnp.where(core == 0, j, (j + OWN) % 96)
        perm = (source[:, None] == jnp.arange(CH)[None, :]).astype(bf16)
        eye = jnp.arange(CH)[:, None] == jnp.arange(CH)[None, :]
        centre = (eye.astype(f32) - 1.0 / CH).astype(bf16)
        zero = jnp.zeros((1,), jnp.int32)
        where = jnp.reshape(chip, (1,)).astype(jnp.int32)
        vectors = jnp.concatenate([b_in.astype(f32) * 0.5] + [v.astype(f32) for v in (ln_in_scale, ln_in_bias, ln_out_scale, ln_out_bias)], axis=1)
        vectors = jnp.broadcast_to(vectors[:, :, None], (2, 1024, CH))
        rows4 = jnp.stack([b_out.astype(f32), b_gate.astype(f32) * 0.5, ln_in_scale.astype(f32), ln_in_bias.astype(f32)], axis=1)
        w_t = jnp.swapaxes(w_in * bf16(0.5), 1, 2)
        tri = (perm, centre, w_out, w_gate * bf16(0.5), vectors, rows4)
        spread = lambda arr: [(arr, i, 0) for i in range(4)]
        a_o, b_o = project(0, [(OWN, spread(z_own), mask_bf, 0)], vectors, w_t, centre, 2, perm)
        b_o2 = swap(b_o, 1)
        own = [(b_o, 0, OWN), (b_o2, 0, OWN)]
        o0, = triangle(0, where, [[(a_o, 0, OWN, z_own, 0, 0)]], own, tri, a_o)
        x1, y2 = swap(o0, 2), swap(o0, 4)
        parts, last = [], o0
        for n in range(2):
            a_n, b_n = project(0, [(16, spread(z_x[n]), mask_x, 16 * n), (16, spread(z_y[n]), mask_y, 16 * n)], vectors, w_t, centre, 2, last)
            b_n2 = swap(b_n, 1)
            parts.append([((a_n, k), (b_n, k), (b_n2, k)) for k in range(2)])
            last = a_n
        piece = lambda n, k, rel: (*parts[n][k][0], 16, (z_x, z_y)[k][n], rel, 0)
        x0, y0 = triangle(0, where, [[piece(0, k, 0), piece(1, k, 0)] for k in range(2)], own, tri, (last, rel), [(OWN, 1, 0, None, None)] * 2)
        a_y, b_y = project(0, [(16, spread(z_y[2]), mask_y, 32)], vectors, w_t, centre, 2, x0)
        b_y2 = swap(b_y, 1)
        a_x, b_x = project(0, [(16, spread(z_x[2]), mask_x, 32)], vectors, w_t, centre, 2, a_y)
        b_x2 = swap(b_x, 1)
        parts.append([((a_x, 0), (b_x, 0), (b_x2, 0)), ((a_y, 0), (b_y, 0), (b_y2, 0))])
        cols = lambda k: [(*p[k][1], 16) for p in parts] + [(*p[k][2], 16) for p in parts]
        piece_x = [piece(n, 0, 2) for n in range(3)]
        last = a_x
        x2, = triangle(0, where, [piece_x], cols(1), tri, last)
        o3 = swap(x2, 2)
        o1, = triangle(0, where, [[(a_o, 0, OWN, z_own, 1, 0)]], cols(0), tri, x2)
        y3 = swap(o1, 4)
        o2, = triangle(0, where, [[(a_o, 0, OWN, z_own, 2, 0)]], cols(1), tri, o1)
        x3 = swap(o2, 2)
        y1 = swap(o3, 4)
        x0, y0 = triangle(0, where, [[piece(2, k, 0)] for k in range(2)], own, tri, o2, [(OWN, 1, 32, None, x0), (OWN, 1, 32, None, y0)])

        tiles = lambda row, *arrs: [(arr, 0, row) for arr in arrs]
        a_o, b_o = project(1, [(OWN, tiles(0, o0, o1, o2, o3), rel, 0)], vectors, w_t, centre, 2, x0, 8)
        b_o2 = swap(b_o, 1)
        a_x, b_x = project(1, [(OWN, tiles(0, x0, x1, x2, x3), rel, OWN)], vectors, w_t, centre, 2, a_o, 8)
        b_x2 = swap(b_x, 1)
        b_ya, = project(1, [(32, tiles(0, y0, y1, y2, y3), rel, 96)], vectors, w_t, centre, 1, a_x)
        b_ya2 = swap(b_ya, 1)
        b_yb, = project(1, [(16, tiles(32, y0, y1, y2, y3), rel, CH)], vectors, w_t, centre, 1, b_ya)
        b_yb2 = swap(b_yb, 1)
        own, col_x = [(b_o, 0, OWN), (b_o2, 0, OWN)], [(b_x, 0, OWN), (b_x2, 0, OWN)]
        col_y = [(b_ya, 0, 32), (b_yb, 0, 16), (b_ya2, 0, 32), (b_yb2, 0, 16)]
        q2, = triangle(1, where, [[(a_x, 0, OWN, x2, None, 0)]], col_y, tri, b_yb)
        p3 = swap(q2, 2)
        out, = triangles(1, where, [
            ([(0, a_o, 0, OWN, o0, None, 0)], own, [(0, 0, 0)]),
            ([(0, a_o, 0, OWN, o1, None, 0)], col_x, [(0, 0, 1)]),
            ([(0, a_o, 0, OWN, o2, None, 0)], col_y, [(0, 0, 2)]),
        ], [(OWN, 4, None)], tri, q2)
        out = lax.dynamic_update_slice(out, p3, (0, chip ^ 3, 0, 0))
        return out.reshape(OWN, 384, CH)

    return jax.shard_map(device_fn, mesh=mesh, in_specs=(row_spec, mask_spec, vec_spec, vec_spec, mat_spec, vec_spec, mat_spec, vec_spec, vec_spec, vec_spec, mat_spec, vec_spec), out_specs=row_spec, check_vma=False)
```

```python
import functools
import jax
import jax.numpy as jnp
from jax import lax
from jax.experimental import pallas as pl
from jax.experimental.pallas import tpu as pltpu
from jax.sharding import PartitionSpec as P

LN_EPS = 1e-5
ROWS = 16
CHUNK = 16
GROUP = 16
PITCH = 136
CH = 128
OWN = 48
VMEM_BYTES = 67043328
ROW_PITCH = 20
NT = (((1,), (1,)), ((), ()))


def norm_sublanes(x, scale, bias):
    mean = jnp.mean(x, axis=0, keepdims=True)
    xc = x - mean
    var = jnp.mean(xc * xc, axis=0, keepdims=True)
    return xc * lax.rsqrt(var + LN_EPS) * scale + bias


def project_kernel(layer, sides, team, sources, *refs):
    z_refs, refs = [refs[4 * n:4 * n + 4] for n in range(len(sources))], refs[4 * len(sources):]
    mask_refs, refs = refs[:len(sources)], refs[len(sources):]
    vectors, w_t, centre_in = refs[:3]
    outs = refs[4:4 + sides]
    proj, znt, stage, keep, bias_ref, ln_s, ln_b, w_ref, centre, zbuf, obuf, load_sem, param_sem, out_sem = refs[4 + sides:]
    rows = sum(n for n, _, _ in sources)
    side0 = 512 - 256 * sides
    moves = [(centre_in, centre), (vectors.at[layer, 512:640], ln_s), (vectors.at[layer, 640:768], ln_b),
             (w_t.at[layer, side0:512], w_ref), (vectors.at[layer, side0:512], bias_ref)]
    at = 0
    for n, (count, _, mask_row) in enumerate(sources):
        moves.append((mask_refs[n].at[mask_row:mask_row + count], keep.at[at:at + count]))
        at += count
    params = [pltpu.make_async_copy(src, dst, param_sem.at[n]) for n, (src, dst) in enumerate(moves)]
    groups = rows // team

    def loads(n, first, g):
        copies = []
        for t in range(4):
            blk, row = sources[n][1][t]
            src = z_refs[n][t].at[pl.ds(pl.multiple_of(row + g * team, team), team), blk]
            dst = zbuf.at[pl.ds(pl.multiple_of(first + g * team, team), team), t]
            copies.append(pltpu.make_async_copy(src, dst, load_sem.at[first // team + g, t]))
        return copies

    for copy in params:
        copy.start()
    first = 0
    for n, (count, _, mask_row) in enumerate(sources):
        def start(g, carry, n=n, first=first):
            for copy in loads(n, first, g):
                copy.start()
            return carry

        lax.fori_loop(0, count // team, start, 0)
        first += count

    def arrive(g):
        for t in range(4):
            dst = zbuf.at[pl.ds(pl.multiple_of(g * team, team), team), t]
            pltpu.make_async_copy(z_refs[0][t].at[0:team, sources[0][1][t][0]], dst, load_sem.at[g, t]).wait()

    def normalise(g):
        z = zbuf[pl.ds(pl.multiple_of(g * team, team), team)].reshape(team * 384, CH)
        xc = lax.dot_general(centre[...], z, NT, preferred_element_type=jnp.float32)
        for lt in range(3 * team):
            ls = slice(lt * CH, lt * CH + CH)
            x = xc[:, ls]
            var = jnp.mean(x * x, axis=0, keepdims=True)
            znt[:, ls] = (x * lax.rsqrt(var + LN_EPS) * ln_s[...] + ln_b[...]).astype(jnp.bfloat16)

    def stores(b, quarter):
        chans = pl.ds(pl.multiple_of(quarter * 32, 32), 32)
        at = pl.ds(pl.multiple_of(b * ROWS, ROWS), ROWS)
        return [pltpu.make_async_copy(obuf.at[b % 2, s, chans], outs[s].at[chans, at], out_sem.at[b % 2, s, quarter]) for s in range(sides)]

    arrive(0)
    for copy in params:
        copy.wait()
    normalise(0)

    def block(b, carry):
        def some(g, carry):
            after = b * (ROWS // team) + g + 1

            @pl.when(after < groups)
            def _():
                arrive(after)

            proj[...] = jnp.dot(w_ref[...], znt[...], preferred_element_type=jnp.float32)
            normalise(jnp.minimum(after, groups - 1))
            for h in range(team):
                i = g * team + h
                for lt in range(3):
                    ls = slice(h * 384 + lt * CH, h * 384 + lt * CH + CH)
                    for s in range(sides):
                        value = proj[s * 256:s * 256 + CH, ls] + bias_ref[s * 256:s * 256 + CH]
                        gate = proj[s * 256 + CH:s * 256 + 256, ls] + bias_ref[s * 256 + CH:s * 256 + 256]
                        stage[s, lt, pl.ds(i, CH, stride=ROW_PITCH), :] = (jnp.tanh(gate) + 1.0) * value
            return carry

        lax.fori_loop(0, ROWS // team, some, 0)

        @pl.when(b >= 2)
        def _():
            for quarter in range(4):
                for copy in stores(b - 2, quarter):
                    copy.wait()

        m = keep[pl.ds(pl.multiple_of(b * ROWS, ROWS), ROWS)]

        def quarter_of(quarter, carry):
            def chan(c8, carry):
                c0 = quarter * 32 + c8 * 8
                for s in range(sides):
                    for lt in range(3):
                        view = stage.at[s, lt, pl.ds(pl.multiple_of(c0 * ROW_PITCH, 8), 8 * ROW_PITCH)]
                        for q in range(8):
                            obuf[b % 2, s, c0 + q, :, lt * CH:lt * CH + CH] = view[q * ROW_PITCH:q * ROW_PITCH + ROWS].astype(jnp.bfloat16) * m[:, lt * CH:lt * CH + CH]
                return carry

            lax.fori_loop(0, 4, chan, 0)
            for copy in stores(b, quarter):
                copy.start()
            return carry

        lax.fori_loop(0, 4, quarter_of, 0)
        return carry

    lax.fori_loop(0, rows // ROWS, block, 0)
    for b in range(max(rows // ROWS - 2, 0), rows // ROWS):
        for quarter in range(4):
            for copy in stores(b, quarter):
                copy.wait()


def project(layer, sources, vectors, w_t, centre, sides, dep, team=4):
    rows = sum(n for n, _, _, _ in sources)
    anywhere = pl.BlockSpec(memory_space=pl.ANY)
    in_specs = [anywhere] * (5 * len(sources) + 4)
    return pl.pallas_call(
        functools.partial(project_kernel, layer, sides, team, [(n, [tile[1:] for tile in tiles], at) for n, tiles, _, at in sources]),
        grid=(1,),
        out_shape=[jax.ShapeDtypeStruct((CH, rows, 384), jnp.bfloat16)] * sides,
        in_specs=in_specs,
        out_specs=[anywhere] * sides,
        scratch_shapes=[pltpu.VMEM((256 * sides, team * 384), jnp.float32), pltpu.VMEM((CH, team * 384), jnp.bfloat16), pltpu.VMEM((sides, 3, CH * ROW_PITCH, CH), jnp.float32), pltpu.VMEM((rows, 384), jnp.bfloat16),
                        pltpu.VMEM((256 * sides, CH), jnp.float32), pltpu.VMEM((CH, CH), jnp.float32), pltpu.VMEM((CH, CH), jnp.float32), pltpu.VMEM((256 * sides, CH), jnp.bfloat16), pltpu.VMEM((CH, CH), jnp.bfloat16),
                        pltpu.VMEM((rows, 4, 96, CH), jnp.bfloat16), pltpu.VMEM((2, sides, CH, ROWS, 384), jnp.bfloat16),
                        pltpu.SemaphoreType.DMA((rows // team, 4)), pltpu.SemaphoreType.DMA((5 + len(sources),)), pltpu.SemaphoreType.DMA((2, sides, 4))],
        compiler_params=pltpu.CompilerParams(dimension_semantics=('arbitrary',), vmem_limit_bytes=VMEM_BYTES),
        cost_estimate=pl.CostEstimate(flops=rows * 384 * CH * 512 * sides, bytes_accessed=rows * 384 * 256 * (1 + sides), transcendentals=0),
        name='project',
    )(*[tile[0] for _, tiles, _, _ in sources for tile in tiles], *[mask for _, _, mask, _ in sources], vectors, w_t, centre, dep)


def triangle_kernel(layer, jobs, n_a, n_b, n_z, n_out, n_held, where_ref, *refs):
    a_refs, refs = refs[:n_a], refs[n_a:]
    b_refs, refs = refs[:n_b], refs[n_b:]
    z_refs, refs = refs[:n_z], refs[n_z:]
    perm_in, centre_in, w_out_in, w_gate_in, vectors, rows_in = refs[:6]
    outs, refs = refs[6 + n_held:6 + n_held + n_out], refs[6 + n_held + n_out:]
    tri, abuf, bbuf, zbuf, obuf, perm_ref, centre, w_out, w_gate, ln_s, ln_b, rows_ref, load_sem, z_sem, param_sem, out_sem = refs
    b_out, b_gate, in_s, in_b = [rows_ref.at[n:n + 1] for n in range(4)]
    moves = [(perm_in, perm_ref), (centre_in, centre), (w_out_in.at[layer], w_out), (w_gate_in.at[layer], w_gate),
             (vectors.at[layer, 768:896], ln_s), (vectors.at[layer, 896:1024], ln_b), (rows_in.at[layer], rows_ref)]
    params = [pltpu.make_async_copy(src, dst, param_sem.at[n]) for n, (src, dst) in enumerate(moves)]
    column = lambda rel: 0 if rel is None else where_ref[0] ^ rel
    regions, z_at, zn, total = {}, [], [], 0
    for pieces, _, _ in jobs:
        z_at.append(total)
        zn.append(sum(len(p) for p, _, _ in jobs[:len(zn)]))
        total += sum(p[3] for p in pieces)

    a_at, loads_a, filled = [], [], 0
    for pieces, _, _ in jobs:
        key = tuple(p[1:4] for p in pieces)
        loads_a.append(key not in regions)
        if key not in regions:
            regions[key] = filled
            filled += sum(p[3] for p in pieces)
        a_at.append(regions[key])

    def loads(j, q):
        pieces, b_pieces, _ = jobs[j]
        chans = pl.ds(pl.multiple_of(q * CHUNK, CHUNK), CHUNK)
        copies, r0 = [], a_at[j]
        for n, (_, a, blk, count, _, _) in enumerate(pieces if loads_a[j] else ()):
            copies.append(pltpu.make_async_copy(a_refs[a].at[chans, blk * count:blk * count + count], abuf.at[chans, r0:r0 + count], load_sem.at[j, q, n]))
            r0 += count
        r0 = 0
        for n, (b, blk, count) in enumerate(b_pieces):
            copies.append(pltpu.make_async_copy(b_refs[b].at[chans, blk * count:blk * count + count], bbuf.at[j, chans, r0:r0 + count], load_sem.at[j, q, len(pieces) + n]))
            r0 += count
        return copies

    def z_loads(j):
        copies, r0 = [], z_at[j]
        for n, (_, _, _, count, rel, z0) in enumerate(jobs[j][0]):
            copies.append(pltpu.make_async_copy(z_refs[zn[j] + n].at[z0:z0 + count, column(rel)], zbuf.at[r0:r0 + count], z_sem.at[zn[j] + n]))
            r0 += count
        return copies

    for j in range(len(jobs)):
        def start_loads(q, carry, j=j):
            for copy in loads(j, q):
                copy.start()
            return carry

        lax.fori_loop(0, CH // CHUNK, start_loads, 0)
        for copy in z_loads(j) + (params if j == 0 else []):
            copy.start()
    tri[:, 96:CH] = jnp.zeros((tri.shape[0], 32), jnp.float32)

    def some_rows(i0, at):
        flipped = []
        for q in range(GROUP):
            o = tri[pl.ds(pl.multiple_of((i0 + q) * PITCH, 8), CH), :]
            on = norm_sublanes(o, ln_s[...], ln_b[...]).astype(jnp.bfloat16)
            flipped.append(lax.dot_general(perm_ref[...], on, NT, preferred_element_type=jnp.float32).astype(jnp.bfloat16))
        on = jnp.concatenate(flipped, axis=0)
        u = jnp.dot(on, w_out[...], preferred_element_type=jnp.float32) + b_out[...]
        u = u.astype(jnp.bfloat16).astype(jnp.float32)
        zb = zbuf[pl.ds(at, GROUP)].reshape(GROUP * 96, CH)
        xc = jnp.dot(zb, centre[...], preferred_element_type=jnp.float32)
        z = zb.astype(jnp.float32)
        var = jnp.mean(xc * xc, axis=-1, keepdims=True)
        zn = (xc * lax.rsqrt(var + LN_EPS) * in_s[...] + in_b[...]).astype(jnp.bfloat16)
        g = jnp.dot(zn, w_gate[...], preferred_element_type=jnp.float32) + b_gate[...]
        g = 0.5 * jnp.tanh(g) + 0.5
        obuf[pl.ds(at, GROUP)] = (z + g * u).astype(jnp.bfloat16).reshape(GROUP, 96, CH)

    written = []
    for j, (pieces, b_pieces, outputs) in enumerate(jobs):
        rows = sum(p[3] for p in pieces)

        def some_channels(q, carry, j=j, rows=rows):
            for copy in loads(j, q):
                copy.wait()
            for cc in range(CHUNK):
                c = q * CHUNK + cc
                o = lax.dot_general(bbuf[j, c], abuf[c, a_at[j]:a_at[j] + rows], NT, preferred_element_type=jnp.float32).T
                tri[pl.ds(c, rows, stride=PITCH), 0:96] = o
            return carry

        lax.fori_loop(0, CH // CHUNK, some_channels, 0)
        for copy in z_loads(j) + (params if j == 0 else []):
            copy.wait()

        spans, r0 = [], 0
        for s, _, _, count, _, _ in pieces:
            if spans and spans[-1][0] == s:
                spans[-1][2] += count
            else:
                spans.append([s, r0, count])
            r0 += count

        def store(s, r0, i, j=j, outputs=outputs):
            arr, first, rel = outputs[s]
            row, to = pl.multiple_of(z_at[j] + r0 + i * GROUP, GROUP), pl.multiple_of(first + i * GROUP, GROUP)
            return pltpu.make_async_copy(obuf.at[pl.ds(row, GROUP)], outs[arr].at[pl.ds(to, GROUP), column(rel)], out_sem.at[(z_at[j] + r0) // GROUP + i])

        for s, r0, count in spans:
            def body(i, carry, s=s, r0=r0, store=store, j=j):
                i0 = pl.multiple_of(r0 + i * GROUP, GROUP)
                some_rows(i0, z_at[j] + i0)
                store(s, r0, i).start()
                return carry

            lax.fori_loop(0, count // GROUP, body, 0)
            written += [(store, s, r0, i) for i in range(count // GROUP)]
    for store, s, r0, i in written:
        store(s, r0, i).wait()


def triangles(layer, where, jobs, arrays, params, dep):
    def place(arr, pool):
        for n, other in enumerate(pool):
            if other is arr:
                return n
        pool.append(arr)
        return len(pool) - 1

    a_pool, b_pool, z_pool, static, most_b, most_a = [], [], [], [], 0, 0
    for pieces, b_pieces, outputs in jobs:
        z_pool += [p[4] for p in pieces]
        static.append(([(p[0], place(p[1], a_pool), p[2], p[3], p[5], p[6]) for p in pieces],
                       [(place(b, b_pool), blk, n) for b, blk, n in b_pieces], outputs))
        most_a, most_b = max(most_a, len(pieces)), max(most_b, len(b_pieces))
    total = sum(p[3] for pieces, _, _ in static for p in pieces)
    rows = max(sum(p[3] for p in pieces) for pieces, _, _ in static)
    keys = {tuple(p[1:4] for p in pieces) for pieces, _, _ in static}
    held_rows = sum(n for key in keys for _, _, n in key)
    deps = dep if isinstance(dep, tuple) else (dep,)
    held = [prev for _, _, prev in arrays if prev is not None]
    first = 1 + len(a_pool) + len(b_pool) + len(z_pool) + len(params) + len(deps)
    aliases, seen = {}, 0
    for s, (_, _, prev) in enumerate(arrays):
        if prev is not None:
            aliases[first + seen] = s
            seen += 1
    anywhere = pl.BlockSpec(memory_space=pl.ANY)
    in_specs = [anywhere] * (len(a_pool) + len(b_pool) + len(z_pool) + len(params) + len(deps) + len(held))
    return pl.pallas_call(
        functools.partial(triangle_kernel, layer, static, len(a_pool), len(b_pool), len(z_pool), len(arrays), len(deps) + len(held)),
        out_shape=[jax.ShapeDtypeStruct((n, width, 96, CH), jnp.bfloat16) for n, width, _ in arrays],
        input_output_aliases=aliases,
        grid_spec=pltpu.PrefetchScalarGridSpec(
            num_scalar_prefetch=1, grid=(1,), in_specs=in_specs, out_specs=[anywhere] * len(arrays),
            scratch_shapes=[pltpu.VMEM((rows * PITCH, CH), jnp.float32), pltpu.VMEM((CH, held_rows, 384), jnp.bfloat16), pltpu.VMEM((len(jobs), CH, 96, 384), jnp.bfloat16),
                            pltpu.VMEM((total, 96, CH), jnp.bfloat16), pltpu.VMEM((total, 96, CH), jnp.bfloat16),
                            pltpu.VMEM((96, CH), jnp.bfloat16), pltpu.VMEM((CH, CH), jnp.bfloat16), pltpu.VMEM((CH, CH), jnp.bfloat16), pltpu.VMEM((CH, CH), jnp.bfloat16),
                            pltpu.VMEM((CH, CH), jnp.float32), pltpu.VMEM((CH, CH), jnp.float32), pltpu.VMEM((4, CH), jnp.float32),
                            pltpu.SemaphoreType.DMA((len(jobs), CH // CHUNK, most_a + most_b)), pltpu.SemaphoreType.DMA((len(z_pool),)), pltpu.SemaphoreType.DMA((7,)), pltpu.SemaphoreType.DMA((total // GROUP,))]),
        compiler_params=pltpu.CompilerParams(dimension_semantics=('arbitrary',), vmem_limit_bytes=VMEM_BYTES),
        cost_estimate=pl.CostEstimate(flops=total * 96 * CH * 1800, bytes_accessed=(total + 96) * 384 * 256, transcendentals=0),
        name='triangle',
    )(where, *a_pool, *b_pool, *z_pool, *params, *deps, *held)


def triangle(layer, where, sets, b_pieces, params, dep, into=None):
    into = into or [(sum(p[2] for p in pieces), 1, 0, None, None) for pieces in sets]
    job = ([(s,) + p for s, pieces in enumerate(sets) for p in pieces], b_pieces, [(s, at, rel) for s, (_, _, at, rel, _) in enumerate(into)])
    return triangles(layer, where, [job], [(n, width, prev) for n, width, _, _, prev in into], params, dep)


def solution(mesh):
    row_spec = P(('batch', 'dap'), None, None)
    mask_spec = P(('batch', 'dap'), None)
    vec_spec = P(None, None)
    mat_spec = P(None, None, None)

    def swap(x, bit):
        return lax.ppermute(x, 'dap', [(i, i ^ bit) for i in range(8)])

    def device_fn(z_rows, mask_rows, ln_in_scale, ln_in_bias, w_in, b_in, w_gate, b_gate, ln_out_scale, ln_out_bias, w_out, b_out):
        f32, bf16 = jnp.float32, jnp.bfloat16
        index = lax.axis_index('dap')
        chip, core = index // 2, index % 2
        z_own = z_rows.reshape(OWN, 4, 96, CH)
        z_x, z_y = [], []
        for n in range(3):
            part = (z_own if n == 0 else lax.optimization_barrier(z_own))[16 * n:16 * n + 16]
            z_x.append(swap(part, 2))
            z_y.append(swap(part, 4))
        mask_bf = mask_rows.astype(bf16)
        mask_x, mask_y = swap(mask_bf, 2), swap(mask_bf, 4)
        masks = [mask_bf, mask_x, mask_y]
        cut = lambda m, n: [m[:, i * n:i * n + n] for i in range(384 // n)]
        rel = jnp.concatenate(masks, axis=0)
        h = cut(rel, 192)
        rel = jnp.where(chip >= 2, jnp.concatenate([h[1], h[0]], axis=1), rel)
        q = cut(rel, 96)
        rel = jnp.where(chip % 2 == 1, jnp.concatenate([q[1], q[0], q[3], q[2]], axis=1), rel)
        j = jnp.arange(96)
        source = jnp.where(core == 0, j, (j + OWN) % 96)
        perm = (source[:, None] == jnp.arange(CH)[None, :]).astype(bf16)
        eye = jnp.arange(CH)[:, None] == jnp.arange(CH)[None, :]
        centre = (eye.astype(f32) - 1.0 / CH).astype(bf16)
        zero = jnp.zeros((1,), jnp.int32)
        where = jnp.reshape(chip, (1,)).astype(jnp.int32)
        vectors = jnp.concatenate([b_in.astype(f32) * 0.5] + [v.astype(f32) for v in (ln_in_scale, ln_in_bias, ln_out_scale, ln_out_bias)], axis=1)
        vectors = jnp.broadcast_to(vectors[:, :, None], (2, 1024, CH))
        rows4 = jnp.stack([b_out.astype(f32), b_gate.astype(f32) * 0.5, ln_in_scale.astype(f32), ln_in_bias.astype(f32)], axis=1)
        w_t = jnp.swapaxes(w_in * bf16(0.5), 1, 2)
        tri = (perm, centre, w_out, w_gate * bf16(0.5), vectors, rows4)
        spread = lambda arr: [(arr, i, 0) for i in range(4)]
        a_o, b_o = project(0, [(OWN, spread(z_own), mask_bf, 0)], vectors, w_t, centre, 2, perm)
        b_o2 = swap(b_o, 1)
        own = [(b_o, 0, OWN), (b_o2, 0, OWN)]
        o0, = triangle(0, where, [[(a_o, 0, OWN, z_own, 0, 0)]], own, tri, a_o)
        x1, y2 = swap(o0, 2), swap(o0, 4)
        parts, last = [], o0
        for n in range(2):
            a_n, b_n = project(0, [(16, spread(z_x[n]), mask_x, 16 * n), (16, spread(z_y[n]), mask_y, 16 * n)], vectors, w_t, centre, 2, last)
            b_n2 = swap(b_n, 1)
            parts.append([((a_n, k), (b_n, k), (b_n2, k)) for k in range(2)])
            last = a_n
        piece = lambda n, k, rel: (*parts[n][k][0], 16, (z_x, z_y)[k][n], rel, 0)
        x0, y0 = triangle(0, where, [[piece(0, k, 0), piece(1, k, 0)] for k in range(2)], own, tri, (last, rel), [(OWN, 1, 0, None, None)] * 2)
        a_y, b_y = project(0, [(16, spread(z_y[2]), mask_y, 32)], vectors, w_t, centre, 2, x0)
        b_y2 = swap(b_y, 1)
        a_x, b_x = project(0, [(16, spread(z_x[2]), mask_x, 32)], vectors, w_t, centre, 2, a_y)
        b_x2 = swap(b_x, 1)
        parts.append([((a_x, 0), (b_x, 0), (b_x2, 0)), ((a_y, 0), (b_y, 0), (b_y2, 0))])
        cols = lambda k: [(*p[k][1], 16) for p in parts] + [(*p[k][2], 16) for p in parts]
        piece_x = [piece(n, 0, 2) for n in range(3)]
        last = a_x
        x2, = triangle(0, where, [piece_x], cols(1), tri, last)
        o3 = swap(x2, 2)
        o1, = triangle(0, where, [[(a_o, 0, OWN, z_own, 1, 0)]], cols(0), tri, x2)
        y3 = swap(o1, 4)
        o2, = triangle(0, where, [[(a_o, 0, OWN, z_own, 2, 0)]], cols(1), tri, o1)
        x3 = swap(o2, 2)
        y1 = swap(o3, 4)
        x0, y0 = triangle(0, where, [[piece(2, k, 0)] for k in range(2)], own, tri, o2, [(OWN, 1, 32, None, x0), (OWN, 1, 32, None, y0)])

        tiles = lambda row, *arrs: [(arr, 0, row) for arr in arrs]
        a_o, b_o = project(1, [(OWN, tiles(0, o0, o1, o2, o3), rel, 0)], vectors, w_t, centre, 2, x0, 8)
        b_o2 = swap(b_o, 1)
        a_x, b_x = project(1, [(OWN, tiles(0, x0, x1, x2, x3), rel, OWN)], vectors, w_t, centre, 2, a_o, 8)
        b_x2 = swap(b_x, 1)
        b_ya, = project(1, [(32, tiles(0, y0, y1, y2, y3), rel, 96)], vectors, w_t, centre, 1, a_x)
        b_ya2 = swap(b_ya, 1)
        b_yb, = project(1, [(16, tiles(32, y0, y1, y2, y3), rel, CH)], vectors, w_t, centre, 1, b_ya)
        b_yb2 = swap(b_yb, 1)
        own, col_x = [(b_o, 0, OWN), (b_o2, 0, OWN)], [(b_x, 0, OWN), (b_x2, 0, OWN)]
        col_y = [(b_ya, 0, 32), (b_yb, 0, 16), (b_ya2, 0, 32), (b_yb2, 0, 16)]
        q2, = triangle(1, where, [[(a_x, 0, OWN, x2, None, 0)]], col_y, tri, b_yb)
        p3 = swap(q2, 2)
        out, = triangles(1, where, [
            ([(0, a_o, 0, OWN, o0, None, 0)], own, [(0, 0, 0)]),
            ([(0, a_o, 0, OWN, o1, None, 0)], col_x, [(0, 0, 1)]),
            ([(0, a_o, 0, OWN, o2, None, 0)], col_y, [(0, 0, 2)]),
        ], [(OWN, 4, None)], tri, q2)
        out = lax.dynamic_update_slice(out, p3, (0, chip ^ 3, 0, 0))
        return out.reshape(OWN, 384, CH)

    return jax.shard_map(device_fn, mesh=mesh, in_specs=(row_spec, mask_spec, vec_spec, vec_spec, mat_spec, vec_spec, mat_spec, vec_spec, vec_spec, vec_spec, mat_spec, vec_spec), out_specs=row_spec, check_vma=False)
```

```python
import functools
import jax
import jax.numpy as jnp
from jax import lax
from jax.experimental import pallas as pl
from jax.experimental.pallas import tpu as pltpu
from jax.sharding import PartitionSpec as P

LN_EPS = 1e-5
ROWS = 16
CHUNK = 16
GROUP = 16
PITCH = 136
CH = 128
OWN = 48
VMEM_BYTES = 67043328
ROW_PITCH = 20
NT = (((1,), (1,)), ((), ()))


def norm_sublanes(x, scale, bias):
    mean = jnp.mean(x, axis=0, keepdims=True)
    xc = x - mean
    var = jnp.mean(xc * xc, axis=0, keepdims=True)
    return xc * lax.rsqrt(var + LN_EPS) * scale + bias


def project_kernel(layer, sides, team, sources, *refs):
    z_refs, refs = [refs[4 * n:4 * n + 4] for n in range(len(sources))], refs[4 * len(sources):]
    mask_refs, refs = refs[:len(sources)], refs[len(sources):]
    vectors, w_t, centre_in = refs[:3]
    outs = refs[4:4 + sides]
    proj, znt, stage, keep, bias_ref, ln_s, ln_b, w_ref, centre, zbuf, obuf, load_sem, param_sem, out_sem = refs[4 + sides:]
    rows = sum(n for n, _, _ in sources)
    side0 = 512 - 256 * sides
    moves = [(centre_in, centre), (vectors.at[layer, 512:640], ln_s), (vectors.at[layer, 640:768], ln_b),
             (w_t.at[layer, side0:512], w_ref), (vectors.at[layer, side0:512], bias_ref)]
    at = 0
    for n, (count, _, mask_row) in enumerate(sources):
        moves.append((mask_refs[n].at[mask_row:mask_row + count], keep.at[at:at + count]))
        at += count
    params = [pltpu.make_async_copy(src, dst, param_sem.at[n]) for n, (src, dst) in enumerate(moves)]
    groups = rows // team

    def loads(n, first, g):
        copies = []
        for t in range(4):
            blk, row = sources[n][1][t]
            src = z_refs[n][t].at[pl.ds(pl.multiple_of(row + g * team, team), team), blk]
            dst = zbuf.at[pl.ds(pl.multiple_of(first + g * team, team), team), t]
            copies.append(pltpu.make_async_copy(src, dst, load_sem.at[first // team + g, t]))
        return copies

    for copy in params:
        copy.start()
    first = 0
    for n, (count, _, mask_row) in enumerate(sources):
        def start(g, carry, n=n, first=first):
            for copy in loads(n, first, g):
                copy.start()
            return carry

        lax.fori_loop(0, count // team, start, 0)
        first += count

    def arrive(g):
        for t in range(4):
            dst = zbuf.at[pl.ds(pl.multiple_of(g * team, team), team), t]
            pltpu.make_async_copy(z_refs[0][t].at[0:team, sources[0][1][t][0]], dst, load_sem.at[g, t]).wait()

    def normalise(g):
        z = zbuf[pl.ds(pl.multiple_of(g * team, team), team)].reshape(team * 384, CH)
        xc = lax.dot_general(centre[...], z, NT, preferred_element_type=jnp.float32)
        for lt in range(3 * team):
            ls = slice(lt * CH, lt * CH + CH)
            x = xc[:, ls]
            var = jnp.mean(x * x, axis=0, keepdims=True)
            znt[:, ls] = (x * lax.rsqrt(var + LN_EPS) * ln_s[...] + ln_b[...]).astype(jnp.bfloat16)

    def stores(b, quarter):
        chans = pl.ds(pl.multiple_of(quarter * 32, 32), 32)
        at = pl.ds(pl.multiple_of(b * ROWS, ROWS), ROWS)
        return [pltpu.make_async_copy(obuf.at[b % 2, s, chans], outs[s].at[chans, at], out_sem.at[b % 2, s, quarter]) for s in range(sides)]

    arrive(0)
    for copy in params:
        copy.wait()
    normalise(0)

    def block(b, carry):
        def some(g, carry):
            after = b * (ROWS // team) + g + 1

            @pl.when(after < groups)
            def _():
                arrive(after)

            proj[...] = jnp.dot(w_ref[...], znt[...], preferred_element_type=jnp.float32)
            normalise(jnp.minimum(after, groups - 1))
            for h in range(team):
                i = g * team + h
                for lt in range(3):
                    ls = slice(h * 384 + lt * CH, h * 384 + lt * CH + CH)
                    for s in range(sides):
                        value = proj[s * 256:s * 256 + CH, ls] + bias_ref[s * 256:s * 256 + CH]
                        gate = proj[s * 256 + CH:s * 256 + 256, ls] + bias_ref[s * 256 + CH:s * 256 + 256]
                        stage[s, lt, pl.ds(i, CH, stride=ROW_PITCH), :] = (jnp.tanh(gate) + 1.0) * value
            return carry

        lax.fori_loop(0, ROWS // team, some, 0)

        @pl.when(b >= 2)
        def _():
            for quarter in range(4):
                for copy in stores(b - 2, quarter):
                    copy.wait()

        m = keep[pl.ds(pl.multiple_of(b * ROWS, ROWS), ROWS)]

        def quarter_of(quarter, carry):
            def chan(c8, carry):
                c0 = quarter * 32 + c8 * 8
                for s in range(sides):
                    for lt in range(3):
                        view = stage.at[s, lt, pl.ds(pl.multiple_of(c0 * ROW_PITCH, 8), 8 * ROW_PITCH)]
                        for q in range(8):
                            obuf[b % 2, s, c0 + q, :, lt * CH:lt * CH + CH] = view[q * ROW_PITCH:q * ROW_PITCH + ROWS].astype(jnp.bfloat16) * m[:, lt * CH:lt * CH + CH]
                return carry

            lax.fori_loop(0, 4, chan, 0)
            for copy in stores(b, quarter):
                copy.start()
            return carry

        lax.fori_loop(0, 4, quarter_of, 0)
        return carry

    lax.fori_loop(0, rows // ROWS, block, 0)
    for b in range(max(rows // ROWS - 2, 0), rows // ROWS):
        for quarter in range(4):
            for copy in stores(b, quarter):
                copy.wait()


def project(layer, sources, vectors, w_t, centre, sides, dep, team=4):
    rows = sum(n for n, _, _, _ in sources)
    anywhere = pl.BlockSpec(memory_space=pl.ANY)
    in_specs = [anywhere] * (5 * len(sources) + 4)
    return pl.pallas_call(
        functools.partial(project_kernel, layer, sides, team, [(n, [tile[1:] for tile in tiles], at) for n, tiles, _, at in sources]),
        grid=(1,),
        out_shape=[jax.ShapeDtypeStruct((CH, rows, 384), jnp.bfloat16)] * sides,
        in_specs=in_specs,
        out_specs=[anywhere] * sides,
        scratch_shapes=[pltpu.VMEM((256 * sides, team * 384), jnp.float32), pltpu.VMEM((CH, team * 384), jnp.bfloat16), pltpu.VMEM((sides, 3, CH * ROW_PITCH, CH), jnp.float32), pltpu.VMEM((rows, 384), jnp.bfloat16),
                        pltpu.VMEM((256 * sides, CH), jnp.float32), pltpu.VMEM((CH, CH), jnp.float32), pltpu.VMEM((CH, CH), jnp.float32), pltpu.VMEM((256 * sides, CH), jnp.bfloat16), pltpu.VMEM((CH, CH), jnp.bfloat16),
                        pltpu.VMEM((rows, 4, 96, CH), jnp.bfloat16), pltpu.VMEM((2, sides, CH, ROWS, 384), jnp.bfloat16),
                        pltpu.SemaphoreType.DMA((rows // team, 4)), pltpu.SemaphoreType.DMA((5 + len(sources),)), pltpu.SemaphoreType.DMA((2, sides, 4))],
        compiler_params=pltpu.CompilerParams(dimension_semantics=('arbitrary',), vmem_limit_bytes=VMEM_BYTES),
        cost_estimate=pl.CostEstimate(flops=rows * 384 * CH * 512 * sides, bytes_accessed=rows * 384 * 256 * (1 + sides), transcendentals=0),
        name='project',
    )(*[tile[0] for _, tiles, _, _ in sources for tile in tiles], *[mask for _, _, mask, _ in sources], vectors, w_t, centre, dep)


def triangle_kernel(layer, chunk, jobs, n_a, n_b, n_z, n_out, n_held, where_ref, *refs):
    a_refs, refs = refs[:n_a], refs[n_a:]
    b_refs, refs = refs[:n_b], refs[n_b:]
    z_refs, refs = refs[:n_z], refs[n_z:]
    perm_in, centre_in, w_out_in, w_gate_in, vectors, rows_in = refs[:6]
    outs, refs = refs[6 + n_held:6 + n_held + n_out], refs[6 + n_held + n_out:]
    tri, abuf, bbuf, zbuf, obuf, perm_ref, centre, w_out, w_gate, ln_s, ln_b, rows_ref, load_sem, z_sem, param_sem, out_sem = refs
    b_out, b_gate, in_s, in_b = [rows_ref.at[n:n + 1] for n in range(4)]
    moves = [(perm_in, perm_ref), (centre_in, centre), (w_out_in.at[layer], w_out), (w_gate_in.at[layer], w_gate),
             (vectors.at[layer, 768:896], ln_s), (vectors.at[layer, 896:1024], ln_b), (rows_in.at[layer], rows_ref)]
    params = [pltpu.make_async_copy(src, dst, param_sem.at[n]) for n, (src, dst) in enumerate(moves)]
    column = lambda rel: 0 if rel is None else where_ref[0] ^ rel
    regions, z_at, zn, total = {}, [], [], 0
    for pieces, _, _ in jobs:
        z_at.append(total)
        zn.append(sum(len(p) for p, _, _ in jobs[:len(zn)]))
        total += sum(p[3] for p in pieces)

    a_at, loads_a, filled = [], [], 0
    for pieces, _, _ in jobs:
        key = tuple(p[1:4] for p in pieces)
        loads_a.append(key not in regions)
        if key not in regions:
            regions[key] = filled
            filled += sum(p[3] for p in pieces)
        a_at.append(regions[key])

    def loads(j, q):
        pieces, b_pieces, _ = jobs[j]
        chans = pl.ds(pl.multiple_of(q * chunk, chunk), chunk)
        copies, r0 = [], a_at[j]
        for n, (_, a, blk, count, _, _) in enumerate(pieces if loads_a[j] else ()):
            copies.append(pltpu.make_async_copy(a_refs[a].at[chans, blk * count:blk * count + count], abuf.at[chans, r0:r0 + count], load_sem.at[j, q, n]))
            r0 += count
        r0 = 0
        for n, (b, blk, count) in enumerate(b_pieces):
            copies.append(pltpu.make_async_copy(b_refs[b].at[chans, blk * count:blk * count + count], bbuf.at[j, chans, r0:r0 + count], load_sem.at[j, q, len(pieces) + n]))
            r0 += count
        return copies

    def z_loads(j):
        copies, r0 = [], z_at[j]
        for n, (_, _, _, count, rel, z0) in enumerate(jobs[j][0]):
            copies.append(pltpu.make_async_copy(z_refs[zn[j] + n].at[z0:z0 + count, column(rel)], zbuf.at[r0:r0 + count], z_sem.at[zn[j] + n]))
            r0 += count
        return copies

    for j in range(len(jobs)):
        def start_loads(q, carry, j=j):
            for copy in loads(j, q):
                copy.start()
            return carry

        lax.fori_loop(0, CH // chunk, start_loads, 0)
        for copy in z_loads(j) + (params if j == 0 else []):
            copy.start()
    tri[:, 96:CH] = jnp.zeros((tri.shape[0], 32), jnp.float32)

    def some_rows(i0, at):
        flipped = []
        for q in range(GROUP):
            o = tri[pl.ds(pl.multiple_of((i0 + q) * PITCH, 8), CH), :]
            on = norm_sublanes(o, ln_s[...], ln_b[...]).astype(jnp.bfloat16)
            flipped.append(lax.dot_general(perm_ref[...], on, NT, preferred_element_type=jnp.float32).astype(jnp.bfloat16))
        on = jnp.concatenate(flipped, axis=0)
        u = jnp.dot(on, w_out[...], preferred_element_type=jnp.float32) + b_out[...]
        u = u.astype(jnp.bfloat16).astype(jnp.float32)
        zb = zbuf[pl.ds(at, GROUP)].reshape(GROUP * 96, CH)
        xc = jnp.dot(zb, centre[...], preferred_element_type=jnp.float32)
        z = zb.astype(jnp.float32)
        var = jnp.mean(xc * xc, axis=-1, keepdims=True)
        zn = (xc * lax.rsqrt(var + LN_EPS) * in_s[...] + in_b[...]).astype(jnp.bfloat16)
        g = jnp.dot(zn, w_gate[...], preferred_element_type=jnp.float32) + b_gate[...]
        g = 0.5 * jnp.tanh(g) + 0.5
        obuf[pl.ds(at, GROUP)] = (z + g * u).astype(jnp.bfloat16).reshape(GROUP, 96, CH)

    written = []
    for j, (pieces, b_pieces, outputs) in enumerate(jobs):
        rows = sum(p[3] for p in pieces)

        def some_channels(q, carry, j=j, rows=rows):
            for copy in loads(j, q):
                copy.wait()
            for cc in range(chunk):
                c = q * chunk + cc
                o = lax.dot_general(bbuf[j, c], abuf[c, a_at[j]:a_at[j] + rows], NT, preferred_element_type=jnp.float32).T
                tri[pl.ds(c, rows, stride=PITCH), 0:96] = o
            return carry

        lax.fori_loop(0, CH // chunk, some_channels, 0)
        for copy in z_loads(j) + (params if j == 0 else []):
            copy.wait()

        spans, r0 = [], 0
        for s, _, _, count, _, _ in pieces:
            if spans and spans[-1][0] == s:
                spans[-1][2] += count
            else:
                spans.append([s, r0, count])
            r0 += count

        def store(s, r0, i, j=j, outputs=outputs):
            arr, first, rel = outputs[s]
            row, to = pl.multiple_of(z_at[j] + r0 + i * GROUP, GROUP), pl.multiple_of(first + i * GROUP, GROUP)
            return pltpu.make_async_copy(obuf.at[pl.ds(row, GROUP)], outs[arr].at[pl.ds(to, GROUP), column(rel)], out_sem.at[(z_at[j] + r0) // GROUP + i])

        for s, r0, count in spans:
            def body(i, carry, s=s, r0=r0, store=store, j=j):
                i0 = pl.multiple_of(r0 + i * GROUP, GROUP)
                some_rows(i0, z_at[j] + i0)
                store(s, r0, i).start()
                return carry

            lax.fori_loop(0, count // GROUP, body, 0)
            written += [(store, s, r0, i) for i in range(count // GROUP)]
    for store, s, r0, i in written:
        store(s, r0, i).wait()


def triangles(layer, where, jobs, arrays, params, dep, chunk=CHUNK):
    def place(arr, pool):
        for n, other in enumerate(pool):
            if other is arr:
                return n
        pool.append(arr)
        return len(pool) - 1

    a_pool, b_pool, z_pool, static, most_b, most_a = [], [], [], [], 0, 0
    for pieces, b_pieces, outputs in jobs:
        z_pool += [p[4] for p in pieces]
        static.append(([(p[0], place(p[1], a_pool), p[2], p[3], p[5], p[6]) for p in pieces],
                       [(place(b, b_pool), blk, n) for b, blk, n in b_pieces], outputs))
        most_a, most_b = max(most_a, len(pieces)), max(most_b, len(b_pieces))
    total = sum(p[3] for pieces, _, _ in static for p in pieces)
    rows = max(sum(p[3] for p in pieces) for pieces, _, _ in static)
    keys = {tuple(p[1:4] for p in pieces) for pieces, _, _ in static}
    held_rows = sum(n for key in keys for _, _, n in key)
    deps = dep if isinstance(dep, tuple) else (dep,)
    held = [prev for _, _, prev in arrays if prev is not None]
    first = 1 + len(a_pool) + len(b_pool) + len(z_pool) + len(params) + len(deps)
    aliases, seen = {}, 0
    for s, (_, _, prev) in enumerate(arrays):
        if prev is not None:
            aliases[first + seen] = s
            seen += 1
    anywhere = pl.BlockSpec(memory_space=pl.ANY)
    in_specs = [anywhere] * (len(a_pool) + len(b_pool) + len(z_pool) + len(params) + len(deps) + len(held))
    return pl.pallas_call(
        functools.partial(triangle_kernel, layer, chunk, static, len(a_pool), len(b_pool), len(z_pool), len(arrays), len(deps) + len(held)),
        out_shape=[jax.ShapeDtypeStruct((n, width, 96, CH), jnp.bfloat16) for n, width, _ in arrays],
        input_output_aliases=aliases,
        grid_spec=pltpu.PrefetchScalarGridSpec(
            num_scalar_prefetch=1, grid=(1,), in_specs=in_specs, out_specs=[anywhere] * len(arrays),
            scratch_shapes=[pltpu.VMEM((rows * PITCH, CH), jnp.float32), pltpu.VMEM((CH, held_rows, 384), jnp.bfloat16), pltpu.VMEM((len(jobs), CH, 96, 384), jnp.bfloat16),
                            pltpu.VMEM((total, 96, CH), jnp.bfloat16), pltpu.VMEM((total, 96, CH), jnp.bfloat16),
                            pltpu.VMEM((96, CH), jnp.bfloat16), pltpu.VMEM((CH, CH), jnp.bfloat16), pltpu.VMEM((CH, CH), jnp.bfloat16), pltpu.VMEM((CH, CH), jnp.bfloat16),
                            pltpu.VMEM((CH, CH), jnp.float32), pltpu.VMEM((CH, CH), jnp.float32), pltpu.VMEM((4, CH), jnp.float32),
                            pltpu.SemaphoreType.DMA((len(jobs), CH // chunk, most_a + most_b)), pltpu.SemaphoreType.DMA((len(z_pool),)), pltpu.SemaphoreType.DMA((7,)), pltpu.SemaphoreType.DMA((total // GROUP,))]),
        compiler_params=pltpu.CompilerParams(dimension_semantics=('arbitrary',), vmem_limit_bytes=VMEM_BYTES),
        cost_estimate=pl.CostEstimate(flops=total * 96 * CH * 1800, bytes_accessed=(total + 96) * 384 * 256, transcendentals=0),
        name='triangle',
    )(where, *a_pool, *b_pool, *z_pool, *params, *deps, *held)


def triangle(layer, where, sets, b_pieces, params, dep, into=None):
    into = into or [(sum(p[2] for p in pieces), 1, 0, None, None) for pieces in sets]
    job = ([(s,) + p for s, pieces in enumerate(sets) for p in pieces], b_pieces, [(s, at, rel) for s, (_, _, at, rel, _) in enumerate(into)])
    return triangles(layer, where, [job], [(n, width, prev) for n, width, _, _, prev in into], params, dep)


def solution(mesh):
    row_spec = P(('batch', 'dap'), None, None)
    mask_spec = P(('batch', 'dap'), None)
    vec_spec = P(None, None)
    mat_spec = P(None, None, None)

    def swap(x, bit):
        return lax.ppermute(x, 'dap', [(i, i ^ bit) for i in range(8)])

    def device_fn(z_rows, mask_rows, ln_in_scale, ln_in_bias, w_in, b_in, w_gate, b_gate, ln_out_scale, ln_out_bias, w_out, b_out):
        f32, bf16 = jnp.float32, jnp.bfloat16
        index = lax.axis_index('dap')
        chip, core = index // 2, index % 2
        z_own = z_rows.reshape(OWN, 4, 96, CH)
        z_x, z_y = [], []
        for n in range(3):
            part = (z_own if n == 0 else lax.optimization_barrier(z_own))[16 * n:16 * n + 16]
            z_x.append(swap(part, 2))
            z_y.append(swap(part, 4))
        mask_bf = mask_rows.astype(bf16)
        mask_x, mask_y = swap(mask_bf, 2), swap(mask_bf, 4)
        masks = [mask_bf, mask_x, mask_y]
        cut = lambda m, n: [m[:, i * n:i * n + n] for i in range(384 // n)]
        rel = jnp.concatenate(masks, axis=0)
        h = cut(rel, 192)
        rel = jnp.where(chip >= 2, jnp.concatenate([h[1], h[0]], axis=1), rel)
        q = cut(rel, 96)
        rel = jnp.where(chip % 2 == 1, jnp.concatenate([q[1], q[0], q[3], q[2]], axis=1), rel)
        j = jnp.arange(96)
        source = jnp.where(core == 0, j, (j + OWN) % 96)
        perm = (source[:, None] == jnp.arange(CH)[None, :]).astype(bf16)
        eye = jnp.arange(CH)[:, None] == jnp.arange(CH)[None, :]
        centre = (eye.astype(f32) - 1.0 / CH).astype(bf16)
        zero = jnp.zeros((1,), jnp.int32)
        where = jnp.reshape(chip, (1,)).astype(jnp.int32)
        vectors = jnp.concatenate([b_in.astype(f32) * 0.5] + [v.astype(f32) for v in (ln_in_scale, ln_in_bias, ln_out_scale, ln_out_bias)], axis=1)
        vectors = jnp.broadcast_to(vectors[:, :, None], (2, 1024, CH))
        rows4 = jnp.stack([b_out.astype(f32), b_gate.astype(f32) * 0.5, ln_in_scale.astype(f32), ln_in_bias.astype(f32)], axis=1)
        w_t = jnp.swapaxes(w_in * bf16(0.5), 1, 2)
        tri = (perm, centre, w_out, w_gate * bf16(0.5), vectors, rows4)
        spread = lambda arr: [(arr, i, 0) for i in range(4)]
        a_o, b_o = project(0, [(OWN, spread(z_own), mask_bf, 0)], vectors, w_t, centre, 2, perm)
        b_o2 = swap(b_o, 1)
        own = [(b_o, 0, OWN), (b_o2, 0, OWN)]
        o0, = triangle(0, where, [[(a_o, 0, OWN, z_own, 0, 0)]], own, tri, a_o)
        x1, y2 = swap(o0, 2), swap(o0, 4)
        parts, last = [], o0
        for n in range(2):
            a_n, b_n = project(0, [(16, spread(z_x[n]), mask_x, 16 * n), (16, spread(z_y[n]), mask_y, 16 * n)], vectors, w_t, centre, 2, last)
            b_n2 = swap(b_n, 1)
            parts.append([((a_n, k), (b_n, k), (b_n2, k)) for k in range(2)])
            last = a_n
        piece = lambda n, k, rel: (*parts[n][k][0], 16, (z_x, z_y)[k][n], rel, 0)
        x0, y0 = triangle(0, where, [[piece(0, k, 0), piece(1, k, 0)] for k in range(2)], own, tri, (last, rel), [(OWN, 1, 0, None, None)] * 2)
        a_y, b_y = project(0, [(16, spread(z_y[2]), mask_y, 32)], vectors, w_t, centre, 2, x0)
        b_y2 = swap(b_y, 1)
        a_x, b_x = project(0, [(16, spread(z_x[2]), mask_x, 32)], vectors, w_t, centre, 2, a_y)
        b_x2 = swap(b_x, 1)
        parts.append([((a_x, 0), (b_x, 0), (b_x2, 0)), ((a_y, 0), (b_y, 0), (b_y2, 0))])
        cols = lambda k: [(*p[k][1], 16) for p in parts] + [(*p[k][2], 16) for p in parts]
        piece_x = [piece(n, 0, 2) for n in range(3)]
        last = a_x
        x2, = triangle(0, where, [piece_x], cols(1), tri, last)
        o3 = swap(x2, 2)
        o1, = triangle(0, where, [[(a_o, 0, OWN, z_own, 1, 0)]], cols(0), tri, x2)
        y3 = swap(o1, 4)
        o2, = triangle(0, where, [[(a_o, 0, OWN, z_own, 2, 0)]], cols(1), tri, o1)
        x3 = swap(o2, 2)
        y1 = swap(o3, 4)
        x0, y0 = triangle(0, where, [[piece(2, k, 0)] for k in range(2)], own, tri, o2, [(OWN, 1, 32, None, x0), (OWN, 1, 32, None, y0)])

        tiles = lambda row, *arrs: [(arr, 0, row) for arr in arrs]
        a_o, b_o = project(1, [(OWN, tiles(0, o0, o1, o2, o3), rel, 0)], vectors, w_t, centre, 2, x0)
        b_o2 = swap(b_o, 1)
        a_x, b_x = project(1, [(OWN, tiles(0, x0, x1, x2, x3), rel, OWN)], vectors, w_t, centre, 2, a_o, 8)
        b_x2 = swap(b_x, 1)
        b_ya, = project(1, [(32, tiles(0, y0, y1, y2, y3), rel, 96)], vectors, w_t, centre, 1, a_x, 8)
        b_ya2 = swap(b_ya, 1)
        b_yb, = project(1, [(16, tiles(32, y0, y1, y2, y3), rel, CH)], vectors, w_t, centre, 1, b_ya)
        b_yb2 = swap(b_yb, 1)
        own, col_x = [(b_o, 0, OWN), (b_o2, 0, OWN)], [(b_x, 0, OWN), (b_x2, 0, OWN)]
        col_y = [(b_ya, 0, 32), (b_yb, 0, 16), (b_ya2, 0, 32), (b_yb2, 0, 16)]
        q2, = triangle(1, where, [[(a_x, 0, OWN, x2, None, 0)]], col_y, tri, b_yb)
        p3 = swap(q2, 2)
        out, = triangles(1, where, [
            ([(0, a_o, 0, OWN, o0, None, 0)], own, [(0, 0, 0)]),
            ([(0, a_o, 0, OWN, o1, None, 0)], col_x, [(0, 0, 1)]),
            ([(0, a_o, 0, OWN, o2, None, 0)], col_y, [(0, 0, 2)]),
        ], [(OWN, 4, None)], tri, q2)
        out = lax.dynamic_update_slice(out, p3, (0, chip ^ 3, 0, 0))
        return out.reshape(OWN, 384, CH)

    return jax.shard_map(device_fn, mesh=mesh, in_specs=(row_spec, mask_spec, vec_spec, vec_spec, mat_spec, vec_spec, mat_spec, vec_spec, vec_spec, vec_spec, mat_spec, vec_spec), out_specs=row_spec, check_vma=False)
```
